1024 devices in a mesh: dp: 8 (over z_lo), seq: 32 (over z_hi, y, core), tensor: 4 (over x).
Axes of the slice: x: 4, y: 4, z: 32 (z_hi: 4, z_lo: 8; z = z_hi * 8 + z_lo), core: 2. Of those that a mesh axis runs over, the one named last changes fastest.
Arguments:
- q_self: bfloat16 [8, 4096, 4096], P('dp', 'seq', 'tensor'), may hold values from -162 to 162
- k_self: bfloat16 [8, 4096, 1024], P('dp', 'seq', 'tensor'), may hold values from -6 to 6
- v_self: bfloat16 [8, 4096, 1024], P('dp', 'seq', 'tensor'), may hold values from -6 to 6
- docs: int32 [8, 4096], P('dp', 'seq'), may hold values from 0 to 31, never falling along the last dimension, each value on 1 to 3072 neighbouring positions
- q_cross: bfloat16 [8, 4096, 4096], P('dp', 'seq', 'tensor'), may hold values from -162 to 162
- cotangent: bfloat16 [8, 4096, 4096], P('dp', 'seq', 'tensor'), may hold values from -6 to 6
- img_keys: bfloat16 [8, 1024, 1024], P('dp', 'seq', 'tensor'), may hold values from -6 to 6
- features: bfloat16 [8, 1024, 1280], P('dp', 'seq'), may hold values from -6 to 6
- w_value: bfloat16 [1280, 1024], P(None, 'tensor'), may hold values from -0.15625 to 0.15625
- tiles: int32 [8, 32], P('dp'), may hold values from 1 to 4
- cite: int32 [8, 32], P('dp'), may hold values from 0 to 31, each once within a row
Outputs:
- combined: bfloat16 [8, 4096, 4096], P('dp', 'seq', 'tensor')
- weight_grad: float32 [1280, 1024], P(('dp', 'seq'), 'tensor')
The draws below stay inside these ranges and needn't reach their ends.
Inputs may be any that keep to these rules, and one draw needn't show every extreme that they name: `docs`: along each sample the document numbers never fall; every document 0 to 31 has one or more tokens. `cite`: each sample's row names every image exactly once.
All inputs are finite; a program needn't handle non-finite values.
Results may differ from the reference program's by a relative error of at most 0.029.
Values may be sent and summed in bfloat16 or wider, within the bound.
A program may use at most 64 MiB of HBM per device.

```python
import math
import jax
import jax.numpy as jnp
import numpy as np
from jax import lax

HEADS = 32
KVH = 8
HD = 128
VIS = 1280
TILES = 4
TILE_TOK = 8
SAMPLES = 8
TOKENS = 4096
IMAGES = 32
DOCS = 32
IMG_TOK = 32


def clipped_normal(seed_key, shape):
    return jnp.clip(jax.random.normal(seed_key, shape, jnp.float32), -6.0, 6.0)


def self_pair(seed_key):
    key_query, key_keys = jax.random.split(seed_key, 2)
    key_field = clipped_normal(key_keys, (SAMPLES, TOKENS, KVH, HD))
    queries = clipped_normal(key_query, (SAMPLES, TOKENS, HEADS, HD))
    return (queries.reshape(SAMPLES, TOKENS, HEADS * HD), key_field.reshape(SAMPLES, TOKENS, KVH * HD))


def cross_pair(seed_key):
    key_query, key_keys = jax.random.split(seed_key, 2)
    slot_count = TILES * TILE_TOK
    key_field = clipped_normal(key_keys, (SAMPLES, IMAGES, slot_count, KVH, HD))
    queries = clipped_normal(key_query, (SAMPLES, TOKENS, HEADS, HD))
    return (queries.reshape(SAMPLES, TOKENS, HEADS * HD), key_field.reshape(SAMPLES, IMAGES * slot_count, KVH * HD))


def draw_q_self(key, part):
    return self_pair(jax.random.fold_in(key, 3))[0].astype(jnp.bfloat16)


def draw_k_self(key, part):
    return self_pair(jax.random.fold_in(key, 3))[1].astype(jnp.bfloat16)


def draw_q_cross(key, part):
    return cross_pair(jax.random.fold_in(key, 5))[0].astype(jnp.bfloat16)


def draw_img_keys(key, part):
    return cross_pair(jax.random.fold_in(key, 5))[1].astype(jnp.bfloat16)


def plant(values, rng, low, high):
    index_at = [jax.random.randint(jax.random.fold_in(rng, axis), (), 0, length) for axis, length in enumerate(values.shape)]
    longest = values.shape.index(max(values.shape))
    next_to = index_at[:longest] + [(index_at[longest] + 1) % values.shape[longest]] + index_at[longest + 1:]
    return values.at[tuple(index_at)].set(low).at[tuple(next_to)].set(high)


def raised(entries, own_key, source, target, blocks, factor):
    owner, partner = [(jnp.arange(entries.shape[axis_at]) // (entries.shape[axis_at] // blocks)).reshape([-1 if axis == axis_at else 1 for axis in range(entries.ndim)]) for axis_at in (source, target)]
    chosen = jax.random.permutation(own_key, blocks)[partner]
    strong = (owner == chosen) | (owner == (partner + blocks // 2) % blocks)
    return jnp.where(strong, factor * entries, entries)


def level_of(own_key, shape, shards, low, largest):
    def one(position, parts):
        heights = jax.random.uniform(jax.random.fold_in(jax.random.fold_in(own_key, 6), position), (parts,), jnp.float32, low / len(shards), largest / len(shards))
        return jnp.repeat(jnp.exp(heights), shape[position] // parts).reshape((-1,) + (1,) * (len(shape) - position - 1))

    gain = one(*shards[0])
    for cut in shards[1:]:
        gain = gain * one(*cut)
    return gain


def split_up(amount, total, limit, skew):
    portions = [(1 << 20) // math.isqrt(grade ** skew) + 1 for grade in range(2, amount + 1)]
    rest, counts = total - limit - (amount - 1), [1] * (amount - 1)
    while rest > 0:
        movable = [i for i in range(amount - 1) if counts[i] < limit]
        mass, remaining = sum([portions[i] for i in movable]), rest
        for i in movable:
            more = min(limit - counts[i], max(1, remaining * portions[i] // mass), rest)
            counts[i] = counts[i] + more
            rest = rest - more
    return np.array([limit] + counts)


def ragged(key, count, total, reach, lean):
    if count == 2:
        one = jax.random.randint(key, (), max(1, total - reach), min(reach, total - 1) + 1)
        return jnp.stack([one, total - one])
    lengths = jnp.asarray(split_up(count, total, reach, lean), jnp.int32)
    couples = (count - 1) // 2
    source_of, taker = lengths[1:1 + 2 * couples:2], lengths[2:2 + 2 * couples:2]
    slack = jnp.minimum(source_of - 1, reach - taker)
    passed = jax.random.randint(jax.random.fold_in(key, 1), (couples,), 0, 1 << 20) % (slack + 1)
    lengths = lengths.at[1:1 + 2 * couples:2].set(source_of - passed).at[2:2 + 2 * couples:2].set(taker + passed)
    return lengths[jax.random.permutation(jax.random.fold_in(key, 2), count)]


def scatter_about(rng, dims, scale, limit, shards=(), held_as=jnp.bfloat16):
    loudness = level_of(rng, dims, shards, -0.22, 0.18) if shards else 1.0
    drawn = jax.random.normal(rng, dims, jnp.float32) * scale * loudness
    return jnp.minimum(jnp.maximum(drawn, -limit), limit).astype(held_as)


def bell_draw_with(own_key, dims, width, most, shards, heavy, kind=jnp.bfloat16):
    result = width * jax.random.normal(own_key, dims, jnp.float32)
    if shards:
        result = result * level_of(own_key, dims, shards, -0.22, 0.18)
    return jnp.clip(raised(result, jax.random.fold_in(own_key, 3), *heavy), -most, most).astype(kind)


def setup_inputs(seed: int = 0) -> dict:
    key_list = jax.random.split(jax.random.key(seed), 12)
    q_self = draw_q_self(jax.random.fold_in(key_list[11], 71), 0)
    k_self = draw_k_self(jax.random.fold_in(key_list[11], 71), 0)
    v_self = scatter_about(key_list[2], (SAMPLES, TOKENS, KVH * HD), 1.0, 6.0, ((0, 8), (1, 32), (2, 4)))
    docs = jax.vmap(lambda own: jnp.searchsorted(jnp.cumsum(ragged(own, DOCS, TOKENS, 3 * TOKENS // 4, 2)), jnp.arange(TOKENS), side="right"))(jax.random.split(key_list[3], SAMPLES)).reshape((SAMPLES, TOKENS)).astype(jnp.int32)
    q_cross = draw_q_cross(jax.random.fold_in(key_list[11], 71), 0)
    cotangent = scatter_about(key_list[5], (SAMPLES, TOKENS, HEADS * HD), 1.0, 6.0, ((0, 8), (1, 32), (2, 4)))
    img_keys = draw_img_keys(jax.random.fold_in(key_list[11], 71), 0)
    features = bell_draw_with(key_list[7], (SAMPLES, IMAGES * IMG_TOK, VIS), 1.0, 6.0, ((0, 8), (1, 32)), (1, 2, 32, 2.75))
    w_value = scatter_about(key_list[8], (VIS, KVH * HD), VIS ** -0.5, 0.15625, ((1, 4),))
    tiles = plant(jax.random.randint(key_list[9], (SAMPLES, IMAGES), 1, TILES + 1), jax.random.fold_in(key_list[9], 1), 1, TILES).astype(jnp.int32)
    cite = jax.vmap(lambda own: jax.random.permutation(own, IMAGES))(jax.random.split(key_list[10], SAMPLES)).reshape((SAMPLES, DOCS)).astype(jnp.int32)
    return dict(q_self=q_self, k_self=k_self, v_self=v_self, docs=docs, q_cross=q_cross, cotangent=cotangent, img_keys=img_keys, features=features, w_value=w_value, tiles=tiles, cite=cite)


MASK_FILL = -1e30


def rounded(values):
    half = lax.optimization_barrier(values.astype(jnp.bfloat16))
    return half.astype(jnp.float32)


def one_sample(q_self, k_self, v_self, docs, q_cross, cotangent, img_keys, features, w_value, tiles, cite):
    tok_count = q_self.shape[0]
    group_size = HEADS // KVH
    score_scale = HD ** -0.5
    key_count = img_keys.shape[0]
    slot_count = key_count // tiles.shape[0]
    values_img = jnp.dot(features, w_value, preferred_element_type=jnp.float32).astype(jnp.bfloat16)
    keys_self = k_self.reshape(tok_count, KVH, HD).astype(jnp.float32)
    vals_self = v_self.reshape(tok_count, KVH, HD).astype(jnp.float32)
    keys_image = img_keys.reshape(key_count, KVH, HD).astype(jnp.float32)
    vals_image = values_img.reshape(key_count, KVH, HD).astype(jnp.float32)
    positions = jnp.arange(tok_count, dtype=jnp.int32)
    slot_ids = jnp.arange(key_count, dtype=jnp.int32)
    key_image = slot_ids // slot_count
    usable = (slot_ids % slot_count) < jnp.repeat(tiles, slot_count, total_repeat_length=key_count) * TILE_TOK
    image_of = cite[docs]
    block_rows = math.gcd(tok_count, 512)

    def block_of(array, offset):
        return lax.dynamic_slice_in_dim(array, offset, block_rows, 0)

    def block_step(grad_sum, offset):
        query_pos = offset + jnp.arange(block_rows, dtype=jnp.int32)
        block_docs = block_of(docs, offset)
        queries = block_of(q_self, offset).reshape(block_rows, KVH, group_size, HD).astype(jnp.float32)
        scores = jnp.einsum("tgcd,sgd->gcts", queries, keys_self) * score_scale
        kept = (query_pos[:, None] >= positions[None, :]) & (block_docs[:, None] == docs[None, :])
        scores = jnp.where(kept, scores, MASK_FILL)
        exp_self = jnp.where(kept, jnp.exp(scores - jnp.max(scores, axis=-1, keepdims=True)), 0.0)
        self_out = jnp.einsum("gcts,sgd->gctd", rounded(exp_self), vals_self) / jnp.sum(exp_self, axis=-1)[..., None]
        cross_q = block_of(q_cross, offset).reshape(block_rows, KVH, group_size, HD).astype(jnp.float32)
        cross_scores = jnp.einsum("tgcd,sgd->gcts", cross_q, keys_image) * score_scale
        cross_kept = (block_of(image_of, offset)[:, None] == key_image[None, :]) & usable[None, :]
        cross_scores = jnp.where(cross_kept, cross_scores, MASK_FILL)
        cross_exp = jnp.where(cross_kept, jnp.exp(cross_scores - jnp.max(cross_scores, axis=-1, keepdims=True)), 0.0)
        cross_weights = rounded(cross_exp / jnp.sum(cross_exp, axis=-1, keepdims=True))
        cross_out = jnp.einsum("gcts,sgd->gctd", cross_weights, vals_image)
        merged = (self_out + cross_out).astype(jnp.bfloat16).transpose(2, 0, 1, 3).reshape(block_rows, HEADS * HD)
        cot_rows = block_of(cotangent, offset).reshape(block_rows, KVH, group_size, HD).astype(jnp.float32)
        grad_sum = grad_sum + jnp.einsum("gcts,tgcd->sgd", cross_weights, cot_rows)
        return grad_sum, merged

    starts = jnp.arange(0, tok_count, block_rows, dtype=jnp.int32)
    grad_sum, out_blocks = lax.scan(block_step, jnp.zeros((key_count, KVH, HD), jnp.float32), starts)
    value_grad = grad_sum.reshape(key_count, KVH * HD).astype(jnp.bfloat16)
    weight_term = jnp.dot(features.T, value_grad, preferred_element_type=jnp.float32)
    return out_blocks.reshape(tok_count, HEADS * HD), weight_term


def reference(q_self, k_self, v_self, docs, q_cross, cotangent, img_keys, features, w_value, tiles, cite):
    outputs = []
    weight_grad = jnp.zeros((VIS, KVH * HD), jnp.float32)
    for sample in range(SAMPLES):
        merged, weight_term = one_sample(q_self[sample], k_self[sample], v_self[sample], docs[sample], q_cross[sample], cotangent[sample], img_keys[sample], features[sample], w_value, tiles[sample], cite[sample])
        outputs.append(merged)
        weight_grad = weight_grad + weight_term
    return jnp.stack(outputs, axis=0), weight_grad
```

```python
import functools
import math

import jax
import jax.numpy as jnp
from jax import lax
from jax.experimental import pallas as pl
from jax.experimental.pallas import tpu as pltpu
from jax.sharding import Mesh
from jax.sharding import PartitionSpec as P

HD = 128
TILE_TOK = 8
IMG_TOK = 32
SEQ = ("seq_0", "seq_1", "seq_2")
DP_SEQ = ("dp", "seq_0", "seq_1", "seq_2")
NEG = -1e30
MESH = pl.DeviceIdType.MESH
SCORE = HD**-0.5 * math.log2(math.e)

OFF = (0, 3, 1, 2)
DOC, KEY, VAL = 0, 1, 2


def kernel(
    q_hbm, k_hbm, v_hbm, docs_hbm, qx_hbm, ct_hbm, ik_hbm, f_hbm, w_hbm, tiles_ref, cite_ref,
    out_ref, wg_ref,
    q, qx, ct, feat, w,
    kv, im, dg, fs, gf, gs, gr, zs, zr, vga, fw, fr,
    m_s, l_s, acc, xc, qd, lo, hi, vacc,
    lsem,
    zs_d, zr_d, zs_i, zr_i, zs_k, zr_k,
    ys_d, yr_d, ys_i, yr_i, ys_k, yr_k,
    cs, cr, fss, fsr, gss, gsr, rss, rsr, vss, vsr, wss, wsr,
):
    b = lax.axis_index("dp")
    h = lax.axis_index("seq_0")
    y = lax.axis_index("seq_1")
    c = lax.axis_index("seq_2")
    yc = y * 2 + c
    own = h * 8 + yc
    pz = h * 8 + b
    up, down, far = (h + 1) % 4, (h + 3) % 4, (h + 2) % 4
    right, left, across = (y + 1) % 4, (y + 3) % 4, (y + 2) % 4
    chunk = (h, down, up, far)
    sends = []

    def remote(src, dst, ss, rs, **where):
        return pltpu.make_async_remote_copy(
            src_ref=src, dst_ref=dst, send_sem=ss, recv_sem=rs, device_id=where, device_id_type=MESH
        )

    def send(src, dst, ss, rs, **where):
        copy = remote(src, dst, ss, rs, **where)
        copy.start()
        sends.append(copy)

    def arrive(dst, ss, rs):
        remote(dst, dst, ss, rs, seq_2=1 - c).wait_recv()

    def yc_of(delta):
        other = (yc + delta) % 8
        return other // 2, other % 2

    def z_of(delta):
        other = (pz + delta) % 32
        return other // 8, other % 8

    local = []

    def fetch(src, dst):
        copy = pltpu.make_async_copy(src, dst, lsem.at[len(local)])
        copy.start()
        local.append(copy)
        return copy

    got_f = fetch(f_hbm.at[0], feat)
    got_w = fetch(w_hbm, w)
    first = [
        fetch(docs_hbm, dg.at[c, h, y]),
        fetch(ik_hbm.at[0], im.at[c, h, y, 0]),
        fetch(k_hbm.at[0], kv.at[c, h, y, 0]),
        fetch(v_hbm.at[0], kv.at[c, h, y, 1]),
    ]
    rest = [fetch(q_hbm.at[0], q), fetch(qx_hbm.at[0], qx), fetch(ct_hbm.at[0], ct)]

    barrier = pltpu.get_barrier_semaphore()
    for delta in (16, *range(1, 16), *range(17, 32)):
        hh, bb = z_of(delta)
        pl.semaphore_signal(barrier, inc=1, device_id={"seq_0": hh, "dp": bb}, device_id_type=MESH)
    for delta in range(1, 8):
        yy, cc = yc_of(delta)
        pl.semaphore_signal(barrier, inc=1, device_id={"seq_1": yy, "seq_2": cc}, device_id_type=MESH)

    got_f.wait()
    got_w.wait()
    im[c, h, y, 1] = jnp.dot(feat[...], w[...], preferred_element_type=jnp.float32).astype(jnp.bfloat16)

    col = lax.broadcasted_iota(jnp.int32, (1, 256), 1)
    wanted = jnp.where(col % 8 < 5, (col // 8) * 40 + col % 8, -1000)
    vis_at = lax.broadcasted_iota(jnp.int32, (1280, 256), 0)

    def pick(partner, _):
        chosen = jnp.where(vis_at == wanted + partner * 5, 1.0, 0.0).astype(jnp.bfloat16)
        fs[partner] = jnp.dot(feat[...], chosen, preferred_element_type=jnp.float32).astype(jnp.bfloat16)
        return 0

    lax.fori_loop(0, 8, pick, 0)
    gf[yc] = fs[yc]

    m_s[...] = jnp.full_like(m_s, NEG)
    l_s[...] = jnp.zeros_like(l_s)
    acc[...] = jnp.zeros_like(acc)
    xc[...] = jnp.zeros_like(xc)

    for copy in first:
        copy.wait()
    my_docs = jnp.broadcast_to(dg[c, h, y].astype(jnp.float32), (128, 128)).T
    qd[...] = my_docs
    number = lax.broadcasted_iota(jnp.int32, (128, 32), 1).astype(jnp.float32)
    cites = jnp.broadcast_to(cite_ref[...].astype(jnp.float32), (128, 32))
    counts = jnp.broadcast_to(tiles_ref[...].astype(jnp.float32), (128, 32))
    image = jnp.sum(jnp.where(number == my_docs[:, :32], cites, 0.0), axis=1, keepdims=True)
    tile_count = jnp.sum(jnp.where(number == image, counts, 0.0), axis=1, keepdims=True)
    lo[...] = jnp.broadcast_to(image * IMG_TOK, (128, 128))
    hi[...] = jnp.broadcast_to(image * IMG_TOK + tile_count * TILE_TOK, (128, 128))

    pl.semaphore_wait(barrier, 38)

    def doc(hc, yy):
        return dg.at[c, hc, yy]

    def img(hc, yy):
        return im.at[c, hc, yy]

    def item(hc, yy, which):
        return kv.at[c, hc, yy, which]

    def half(hc, which, part):
        return kv.at[c, hc, y, which, pl.ds(part * 64, 64)]

    def z_half(which, part, way):
        n = which * 2 + part
        where = up if way == 0 else down
        send(half(h, which, part), half(h, which, part), zs_k.at[way, n], zr_k.at[way, n], seq_0=where)

    def z_half_in(which, part, way):
        n = which * 2 + part
        hc = down if way == 0 else up
        arrive(half(hc, which, part), zs_k.at[way, n], zr_k.at[way, n])

    def y_first_small(r):
        hc = chunk[r]
        for way, where in ((0, right), (1, left)):
            send(doc(hc, y), doc(hc, y), ys_d.at[r, way], yr_d.at[r, way], seq_1=where)
            send(img(hc, y), img(hc, y), ys_i.at[r, way], yr_i.at[r, way], seq_1=where)

    def y_second_small(r):
        hc = chunk[r]
        arrive(doc(hc, left), ys_d.at[r, 0], yr_d.at[r, 0])
        send(doc(hc, left), doc(hc, left), ys_d.at[r, 2], yr_d.at[r, 2], seq_1=right)
        arrive(img(hc, left), ys_i.at[r, 0], yr_i.at[r, 0])
        send(img(hc, left).at[0], img(hc, left).at[0], ys_i.at[r, 2], yr_i.at[r, 2], seq_1=right)
        arrive(doc(hc, right), ys_d.at[r, 1], yr_d.at[r, 1])
        arrive(img(hc, right), ys_i.at[r, 1], yr_i.at[r, 1])
        send(img(hc, right).at[1], img(hc, right).at[1], ys_i.at[r, 3], yr_i.at[r, 3], seq_1=left)

    def core_small(r):
        hc = chunk[r]
        arrive(doc(hc, across), ys_d.at[r, 2], yr_d.at[r, 2])
        send(dg.at[c, hc], dg.at[c, hc], cs.at[DOC, r], cr.at[DOC, r], seq_2=1 - c)
        arrive(img(hc, across).at[0], ys_i.at[r, 2], yr_i.at[r, 2])
        arrive(img(hc, across).at[1], ys_i.at[r, 3], yr_i.at[r, 3])
        send(im.at[c, hc], im.at[c, hc], cs.at[KEY, r], cr.at[KEY, r], seq_2=1 - c)

    def core_small_in(r):
        hc = chunk[r]
        arrive(dg.at[1 - c, hc], cs.at[DOC, r], cr.at[DOC, r])
        arrive(im.at[1 - c, hc], cs.at[KEY, r], cr.at[KEY, r])

    def y_first(r, which):
        hc = chunk[r]
        for way, where in ((0, right), (1, left)):
            send(item(hc, y, which), item(hc, y, which), ys_k.at[r, which, way], yr_k.at[r, which, way], seq_1=where)

    def y_second(r, which):
        hc = chunk[r]
        if which == 0:
            arrive(item(hc, left, 0), ys_k.at[r, 0, 0], yr_k.at[r, 0, 0])
            send(item(hc, left, 0), item(hc, left, 0), ys_k.at[r, 0, 2], yr_k.at[r, 0, 2], seq_1=right)
            arrive(item(hc, right, 0), ys_k.at[r, 0, 1], yr_k.at[r, 0, 1])
        else:
            arrive(item(hc, right, 1), ys_k.at[r, 1, 1], yr_k.at[r, 1, 1])
            send(item(hc, right, 1), item(hc, right, 1), ys_k.at[r, 1, 2], yr_k.at[r, 1, 2], seq_1=left)
            arrive(item(hc, left, 1), ys_k.at[r, 1, 0], yr_k.at[r, 1, 0])

    def core(r):
        hc = chunk[r]
        arrive(item(hc, across, 0), ys_k.at[r, 0, 2], yr_k.at[r, 0, 2])
        arrive(item(hc, across, 1), ys_k.at[r, 1, 2], yr_k.at[r, 1, 2])
        send(kv.at[c, hc], kv.at[c, hc], cs.at[VAL, r], cr.at[VAL, r], seq_2=1 - c)

    def core_in(r):
        hc = chunk[r]
        arrive(kv.at[1 - c, hc], cs.at[VAL, r], cr.at[VAL, r])

    def stacked(ref, g):
        return jnp.concatenate(
            [ref[:, pl.ds(pl.multiple_of(g * 512 + i * 128, 128), 128)] for i in range(4)], axis=0
        )

    def lanes(g):
        return pl.ds(pl.multiple_of(g * 128, 128), 128)

    def cross(r):
        hc = chunk[r]

        def one(g, _):
            keys = jnp.concatenate([im[i, hc, :, 0, :, lanes(g)].reshape(128, 128) for i in (0, 1)], axis=0)
            values = jnp.concatenate([im[i, hc, :, 1, :, lanes(g)].reshape(128, 128) for i in (0, 1)], axis=0)
            s = lax.dot_general(
                stacked(qx, g), keys, (((1,), (1,)), ((), ())), preferred_element_type=jnp.float32
            )
            at = lax.broadcasted_iota(jnp.int32, (1, 256), 1)
            slot = (((hc * 4 + (at % 128) // 32) * 2 + at // 128) * 32 + at % 32).astype(jnp.float32)
            bias = jnp.where((slot >= lo[:, :1]) & (slot < hi[:, :1]), 0.0, NEG)
            s = (s.reshape(4, 128, 256) * SCORE + bias[None]).reshape(512, 256)
            top = jnp.max(s, axis=1, keepdims=True)
            e = jnp.exp2(s - top)
            total = jnp.sum(e, axis=1, keepdims=True)
            weights = (e * jnp.where(top > 0.5 * NEG, 1.0 / total, 0.0)).astype(jnp.bfloat16)
            xc[g] += jnp.dot(weights, values, preferred_element_type=jnp.float32)
            grad = lax.dot_general(
                weights, stacked(ct, g), (((0,), (0,)), ((), ())), preferred_element_type=jnp.float32
            ).astype(jnp.bfloat16)
            for i in (0, 1):
                gs[r, i, :, :, lanes(g)] = grad[i * 128 : (i + 1) * 128].reshape(4, 32, 128)
            return 0

        lax.fori_loop(0, 2, one, 0)

    def attend(r):
        hc = chunk[r]

        def one(n, _):
            g, half_at = n // 2, n % 2
            keys = kv[half_at, hc, :, 0, :, lanes(g)].reshape(512, 128)
            values = kv[half_at, hc, :, 1, :, lanes(g)].reshape(512, 128)
            s = lax.dot_general(
                stacked(q, g), keys, (((1,), (1,)), ((), ())), preferred_element_type=jnp.float32
            )
            key_doc = jnp.concatenate([dg[half_at, hc, i] for i in range(4)], axis=1).astype(jnp.float32)
            at = lax.broadcasted_iota(jnp.int32, (128, 512), 1)
            key_pos = ((hc * 4 + at // 128) * 2 + half_at) * 128 + at % 128
            row_pos = own * 128 + lax.broadcasted_iota(jnp.int32, (128, 512), 0)
            bias = jnp.where((key_doc == qd[:, :1]) & (key_pos <= row_pos), 0.0, NEG)
            s = (s.reshape(4, 128, 512) * SCORE + bias[None]).reshape(512, 512)
            old = m_s[g][:, :1]
            top = jnp.maximum(old, jnp.max(s, axis=1, keepdims=True))
            e = jnp.exp2(s - top)
            fade = jnp.exp2(old - top)
            m_s[g] = jnp.broadcast_to(top, (512, 128))
            l_s[g] = l_s[g] * fade + jnp.broadcast_to(jnp.sum(e, axis=1, keepdims=True), (512, 128))
            acc[g] = acc[g] * fade + jnp.dot(e.astype(jnp.bfloat16), values, preferred_element_type=jnp.float32)
            return 0

        lax.fori_loop(0, 4, one, 0)

    def grad_out(r):
        for delta in range(1, 8):
            yy, cc = yc_of(delta)
            send(gs.at[r, cc, yy], gr.at[r, delta], gss.at[r, delta], gsr.at[r, delta], seq_1=yy, seq_2=cc)

    def grad_in(r):
        total = gs[r, c, y].astype(jnp.float32)
        for delta in range(1, 8):
            arrive(gr.at[r, delta], gss.at[r, delta], gsr.at[r, delta])
        for delta in range(1, 8):
            total += gr[r, delta].astype(jnp.float32)
        return total

    def owner_out(r):
        zs[r] = grad_in(r).astype(jnp.bfloat16)
        send(zs.at[r], zr.at[r], rss.at[r], rsr.at[r], seq_0=chunk[r])

    for way, where in ((0, up), (1, down)):
        send(doc(h, y), doc(h, y), zs_d.at[way], zr_d.at[way], seq_0=where)
        send(img(h, y), img(h, y), zs_i.at[way], zr_i.at[way], seq_0=where)
    z_half(0, 0, 0)
    z_half(1, 0, 1)
    y_first_small(0)
    for delta in range(1, 8):
        yy, cc = yc_of(delta)
        send(fs.at[yy * 2 + cc], gf.at[yc], fss.at[delta], fsr.at[delta], seq_1=yy, seq_2=cc)
    y_first(0, 0)
    y_first(0, 1)
    for copy in rest:
        copy.wait()

    y_second_small(0)
    core_small(0)
    y_second(0, 0)
    y_second(0, 1)
    core_small_in(0)
    cross(0)
    grad_out(0)
    core(0)

    arrive(doc(down, y), zs_d.at[0], zr_d.at[0])
    send(doc(down, y), doc(down, y), zs_d.at[2], zr_d.at[2], seq_0=up)
    arrive(img(down, y), zs_i.at[0], zr_i.at[0])
    send(img(down, y).at[0], img(down, y).at[0], zs_i.at[2], zr_i.at[2], seq_0=up)
    arrive(doc(up, y), zs_d.at[1], zr_d.at[1])
    arrive(img(up, y), zs_i.at[1], zr_i.at[1])
    send(img(up, y).at[1], img(up, y).at[1], zs_i.at[3], zr_i.at[3], seq_0=down)
    z_half(0, 1, 0)
    z_half(1, 1, 1)
    z_half(1, 0, 0)
    z_half(0, 0, 1)
    z_half(1, 1, 0)
    z_half(0, 1, 1)
    y_first_small(1)
    y_first_small(2)
    core_in(0)
    attend(0)
    y_second_small(1)
    y_second_small(2)
    core_small(1)
    core_small(2)
    vacc[...] = grad_in(0)
    core_small_in(1)
    cross(1)
    grad_out(1)
    core_small_in(2)
    cross(2)
    grad_out(2)

    arrive(doc(far, y), zs_d.at[2], zr_d.at[2])
    arrive(img(far, y).at[0], zs_i.at[2], zr_i.at[2])
    arrive(img(far, y).at[1], zs_i.at[3], zr_i.at[3])
    y_first_small(3)
    owner_out(1)
    owner_out(2)
    y_second_small(3)
    core_small(3)
    core_small_in(3)
    cross(3)
    grad_out(3)

    z_half_in(0, 0, 0)
    z_half_in(0, 1, 0)
    send(item(down, y, 0), item(down, y, 0), zs_k.at[0, 4], zr_k.at[0, 4], seq_0=up)
    y_first(1, 0)
    z_half_in(1, 0, 1)
    z_half_in(1, 1, 1)
    send(item(up, y, 1), item(up, y, 1), zs_k.at[1, 4], zr_k.at[1, 4], seq_0=down)
    y_first(2, 1)
    owner_out(3)
    y_second(1, 0)
    y_second(2, 1)
    z_half_in(1, 0, 0)
    z_half_in(1, 1, 0)
    y_first(1, 1)
    z_half_in(0, 0, 1)
    z_half_in(0, 1, 1)
    y_first(2, 0)
    y_second(1, 1)
    core(1)
    y_second(2, 0)
    core(2)

    total = vacc[...]
    for r in (1, 2, 3):
        arrive(zr.at[r], rss.at[r], rsr.at[r])
    for r in (1, 2, 3):
        total += zr[r].astype(jnp.float32)
    vga[yc] = total.astype(jnp.bfloat16)
    for delta in range(1, 8):
        yy, cc = yc_of(delta)
        send(vga.at[yc], vga.at[yc], vss.at[delta], vsr.at[delta], seq_1=yy, seq_2=cc)
    core_in(1)
    pl.when(chunk[1] < h)(lambda: attend(1))

    for delta in range(1, 8):
        yy, cc = yc_of(8 - delta)
        arrive(gf.at[yy * 2 + cc], fss.at[delta], fsr.at[delta])
        arrive(vga.at[yy * 2 + cc], vss.at[delta], vsr.at[delta])
    term = lax.dot_general(
        gf[...].reshape(256, 256), vga[...].reshape(256, 256), (((0,), (0,)), ((), ())),
        preferred_element_type=jnp.float32,
    )
    fw[...] = jnp.concatenate(
        [term[:, :128].reshape(32, 8, 128), term[:, 128:].reshape(32, 8, 128)], axis=1
    ).astype(jnp.bfloat16)
    for delta in sorted(range(1, 32), key=lambda d: abs(d - 16)):
        hh, bb = z_of(delta)
        send(fw.at[bb * 4 + hh], fr.at[delta], wss.at[delta], wsr.at[delta], seq_0=hh, dp=bb)
    core_in(2)
    pl.when(chunk[2] < h)(lambda: attend(2))

    arrive(item(far, y, 0), zs_k.at[0, 4], zr_k.at[0, 4])
    y_first(3, 0)
    arrive(item(far, y, 1), zs_k.at[1, 4], zr_k.at[1, 4])
    y_first(3, 1)
    y_second(3, 0)
    y_second(3, 1)
    core(3)
    core_in(3)
    pl.when(chunk[3] < h)(lambda: attend(3))

    for g in range(2):
        out = (acc[g] / l_s[g] + xc[g]).astype(jnp.bfloat16)
        for i in range(4):
            out_ref[0, :, (g * 4 + i) * 128 : (g * 4 + i + 1) * 128] = out[i * 128 : (i + 1) * 128]

    whole = fw[b * 4 + h].astype(jnp.float32)
    for delta in range(1, 32):
        arrive(fr.at[delta], wss.at[delta], wsr.at[delta])
    for delta in range(1, 32):
        whole += fr[delta].astype(jnp.float32)
    wg_ref[:, :128] = whole[:5]
    wg_ref[:, 128:] = whole[8:13]
    for copy in sends:
        copy.wait_send()


def on_device(*args):
    bf, f32, i32 = jnp.bfloat16, jnp.float32, jnp.int32
    any_space = pl.BlockSpec(memory_space=pl.ANY)
    vmem = pl.BlockSpec(memory_space=pltpu.VMEM)
    V, D = pltpu.VMEM, pltpu.SemaphoreType.DMA
    pairs = [(3,), (4,), (2, 5), (4, 3), (4, 4), (4, 2, 3), (3, 4), (8,), (4, 8), (4,), (8,), (32,)]
    return pl.pallas_call(
        kernel,
        out_shape=(
            jax.ShapeDtypeStruct((1, 128, 1024), bf),
            jax.ShapeDtypeStruct((5, 256), f32),
        ),
        in_specs=[any_space] * 9 + [vmem] * 2,
        out_specs=(vmem, vmem),
        scratch_shapes=[
            V((128, 1024), bf), V((128, 1024), bf), V((128, 1024), bf), V((32, 1280), bf), V((1280, 256), bf),
            V((2, 4, 4, 2, 128, 256), bf), V((2, 4, 4, 2, 32, 256), bf), V((2, 4, 4, 1, 128), i32),
            V((8, 32, 256), bf), V((8, 32, 256), bf),
            V((4, 2, 4, 32, 256), bf), V((4, 8, 32, 256), bf),
            V((4, 32, 256), bf), V((4, 32, 256), bf),
            V((8, 32, 256), bf), V((32, 16, 128), bf), V((32, 16, 128), bf),
            V((2, 512, 128), f32), V((2, 512, 128), f32), V((2, 512, 128), f32), V((2, 512, 128), f32),
            V((128, 128), f32), V((128, 128), f32), V((128, 128), f32), V((32, 256), f32),
            D((9,)),
        ]
        + [D(shape) for shape in pairs for _ in (0, 1)],
        compiler_params=pltpu.CompilerParams(
            collective_id=0, has_side_effects=True, vmem_limit_bytes=48 * 1024 * 1024
        ),
    )(*args)


def solution(mesh):
    split = Mesh(
        mesh.devices.reshape(mesh.shape["dp"], 4, 4, 2, mesh.shape["tensor"]),
        ("dp", "seq_0", "seq_1", "seq_2", "tensor"),
    )
    placed = (
        P("dp", SEQ, "tensor"),
        P("dp", SEQ, "tensor"),
        P("dp", SEQ, "tensor"),
        P("dp", SEQ),
        P("dp", SEQ, "tensor"),
        P("dp", SEQ, "tensor"),
        P("dp", SEQ, "tensor"),
        P("dp", SEQ, None),
        P(None, "tensor"),
        P("dp", None),
        P("dp", None),
    )
    return jax.shard_map(
        on_device,
        mesh=split,
        in_specs=placed,
        out_specs=(P("dp", SEQ, "tensor"), P(DP_SEQ, "tensor")),
        check_vma=False,
    )
```

```python
import functools
import math

import jax
import jax.numpy as jnp
from jax import lax
from jax.experimental import pallas as pl
from jax.experimental.pallas import tpu as pltpu
from jax.sharding import Mesh
from jax.sharding import PartitionSpec as P

HD = 128
TILE_TOK = 8
IMG_TOK = 32
SEQ = ("seq_0", "seq_1", "seq_2")
DP_SEQ = ("dp", "seq_0", "seq_1", "seq_2")
NEG = -1e30
MESH = pl.DeviceIdType.MESH
SCORE = HD**-0.5 * math.log2(math.e)

OFF = (0, 3, 1, 2)
DOC, KEY, VAL = 0, 1, 2


def kernel(
    q_hbm, k_hbm, v_hbm, docs_hbm, qx_hbm, ct_hbm, ik_hbm, f_hbm, w_hbm, tiles_ref, cite_ref,
    out_ref, wg_ref,
    q, qx, ct, feat, w,
    kv, im, dg, fs, gf, gs, gr, zs, zr, vga, fw, fr,
    m_s, l_s, acc, xc, qd, lo, hi, vacc,
    lsem,
    zs_d, zr_d, zs_i, zr_i, zs_k, zr_k,
    ys_d, yr_d, ys_i, yr_i, ys_k, yr_k,
    cs, cr, fss, fsr, gss, gsr, rss, rsr, vss, vsr, wss, wsr,
):
    b = lax.axis_index("dp")
    h = lax.axis_index("seq_0")
    y = lax.axis_index("seq_1")
    c = lax.axis_index("seq_2")
    yc = y * 2 + c
    own = h * 8 + yc
    pz = h * 8 + b
    up, down, far = (h + 1) % 4, (h + 3) % 4, (h + 2) % 4
    right, left, across = (y + 1) % 4, (y + 3) % 4, (y + 2) % 4
    chunk = (h, down, up, far)
    mate = 1 - c
    conds = {
        "all": None,
        "up": h <= 2,
        "low": h <= 1,
        "first": h == 0,
        "mid": (h == 1) | (h == 2),
        "ends": (h == 0) | (h == 3),
        1: h >= 1,
        2: h == 3,
        3: h >= 2,
    }
    sends = {key: [] for key in conds}
    now = ["all"]

    def on(key, *steps):
        def run():
            now[0] = key
            for step in steps:
                step()
            now[0] = "all"

        pl.when(conds[key])(run)

    def at(ref, *index):
        return ref, index

    def remote(*parts, **where):
        src, dst, ss, rs = (ref.at[index] for ref, index in parts)
        return pltpu.make_async_remote_copy(
            src_ref=src, dst_ref=dst, send_sem=ss, recv_sem=rs, device_id=where, device_id_type=MESH
        )

    def send(src, dst, ss, rs, **where):
        remote(src, dst, ss, rs, **where).start()
        sends[now[0]].append(lambda: remote(src, dst, ss, rs, **where))

    def arrive(dst, ss, rs):
        remote(dst, dst, ss, rs, seq_2=mate).wait_recv()

    def yc_of(delta):
        other = (yc + delta) % 8
        return other // 2, other % 2

    def z_of(delta):
        other = (pz + delta) % 32
        return other // 8, other % 8

    local = []

    def fetch(src, dst):
        copy = pltpu.make_async_copy(src, dst, lsem.at[len(local)])
        copy.start()
        local.append(copy)
        return copy

    got_f = fetch(f_hbm.at[0], feat)
    got_w = fetch(w_hbm, w)
    first = [
        fetch(docs_hbm, dg.at[c, h, y]),
        fetch(ik_hbm.at[0], im.at[c, h, y, 0]),
        fetch(k_hbm.at[0], kv.at[c, h, y, 0]),
        fetch(v_hbm.at[0], kv.at[c, h, y, 1]),
    ]
    rest = [fetch(q_hbm.at[0], q), fetch(qx_hbm.at[0], qx), fetch(ct_hbm.at[0], ct)]

    barrier = pltpu.get_barrier_semaphore()
    for where in (up, down):
        pl.semaphore_signal(barrier, inc=1, device_id={"seq_0": where}, device_id_type=MESH)
    for delta in range(1, 8):
        pl.semaphore_signal(barrier, inc=1, device_id={"dp": (b + delta) % 8}, device_id_type=MESH)
    for delta in range(1, 8):
        yy, cc = yc_of(delta)
        pl.semaphore_signal(barrier, inc=1, device_id={"seq_1": yy, "seq_2": cc}, device_id_type=MESH)

    got_f.wait()
    got_w.wait()
    im[c, h, y, 1] = jnp.dot(feat[...], w[...], preferred_element_type=jnp.float32).astype(jnp.bfloat16)

    col = lax.broadcasted_iota(jnp.int32, (1, 256), 1)
    wanted = jnp.where(col % 8 < 5, (col // 8) * 40 + col % 8, -1000)
    vis_at = lax.broadcasted_iota(jnp.int32, (1280, 256), 0)

    def pick(partner, _):
        chosen = jnp.where(vis_at == wanted + partner * 5, 1.0, 0.0).astype(jnp.bfloat16)
        fs[partner] = jnp.dot(feat[...], chosen, preferred_element_type=jnp.float32).astype(jnp.bfloat16)
        return 0

    lax.fori_loop(0, 8, pick, 0)
    gf[yc] = fs[yc]

    m_s[...] = jnp.full_like(m_s, NEG)
    l_s[...] = jnp.zeros_like(l_s)
    acc[...] = jnp.zeros_like(acc)
    xc[...] = jnp.zeros_like(xc)

    for copy in first:
        copy.wait()
    my_docs = jnp.broadcast_to(dg[c, h, y].astype(jnp.float32), (128, 128)).T
    qd[...] = my_docs
    number = lax.broadcasted_iota(jnp.int32, (128, 32), 1).astype(jnp.float32)
    cites = jnp.broadcast_to(cite_ref[...].astype(jnp.float32), (128, 32))
    counts = jnp.broadcast_to(tiles_ref[...].astype(jnp.float32), (128, 32))
    image = jnp.sum(jnp.where(number == my_docs[:, :32], cites, 0.0), axis=1, keepdims=True)
    tile_count = jnp.sum(jnp.where(number == image, counts, 0.0), axis=1, keepdims=True)
    lo[...] = jnp.broadcast_to(image * IMG_TOK, (128, 128))
    hi[...] = jnp.broadcast_to(image * IMG_TOK + tile_count * TILE_TOK, (128, 128))

    pl.semaphore_wait(barrier, 16)

    def doc(hc, yy):
        return at(dg, c, hc, yy)

    def img(hc, yy, *part):
        return at(im, c, hc, yy, *part)

    def item(hc, yy, which):
        return at(kv, c, hc, yy, which)

    def half(hc, which, part):
        return at(kv, c, hc, y, which, pl.ds(part * 64, 64))

    def z_half(which, part, way):
        n = which * 2 + part
        where = up if way == 0 else down
        send(half(h, which, part), half(h, which, part), at(zs_k, way, n), at(zr_k, way, n), seq_0=where)

    def z_half_in(which, part, way):
        n = which * 2 + part
        hc = down if way == 0 else up
        arrive(half(hc, which, part), at(zs_k, way, n), at(zr_k, way, n))

    def y_first_small(r):
        hc = chunk[r]
        for way, where in ((0, right), (1, left)):
            send(doc(hc, y), doc(hc, y), at(ys_d, r, way), at(yr_d, r, way), seq_1=where)
            send(img(hc, y), img(hc, y), at(ys_i, r, way), at(yr_i, r, way), seq_1=where)

    def y_second_small(r):
        hc = chunk[r]
        arrive(doc(hc, left), at(ys_d, r, 0), at(yr_d, r, 0))
        send(doc(hc, left), doc(hc, left), at(ys_d, r, 2), at(yr_d, r, 2), seq_1=right)
        arrive(img(hc, left), at(ys_i, r, 0), at(yr_i, r, 0))
        send(img(hc, left, 0), img(hc, left, 0), at(ys_i, r, 2), at(yr_i, r, 2), seq_1=right)
        arrive(doc(hc, right), at(ys_d, r, 1), at(yr_d, r, 1))
        arrive(img(hc, right), at(ys_i, r, 1), at(yr_i, r, 1))
        send(img(hc, right, 1), img(hc, right, 1), at(ys_i, r, 3), at(yr_i, r, 3), seq_1=left)

    def core_small(r):
        hc = chunk[r]
        arrive(doc(hc, across), at(ys_d, r, 2), at(yr_d, r, 2))
        send(at(dg, c, hc), at(dg, c, hc), at(cs, DOC, r), at(cr, DOC, r), seq_2=mate)
        arrive(img(hc, across, 0), at(ys_i, r, 2), at(yr_i, r, 2))
        arrive(img(hc, across, 1), at(ys_i, r, 3), at(yr_i, r, 3))
        send(at(im, c, hc), at(im, c, hc), at(cs, KEY, r), at(cr, KEY, r), seq_2=mate)

    def core_small_in(r):
        hc = chunk[r]
        arrive(at(dg, mate, hc), at(cs, DOC, r), at(cr, DOC, r))
        arrive(at(im, mate, hc), at(cs, KEY, r), at(cr, KEY, r))

    def y_first(r, which):
        hc = chunk[r]
        for way, where in ((0, right), (1, left)):
            send(item(hc, y, which), item(hc, y, which), at(ys_k, r, which, way), at(yr_k, r, which, way), seq_1=where)

    def y_second(r, which):
        hc = chunk[r]
        if which == 0:
            arrive(item(hc, left, 0), at(ys_k, r, 0, 0), at(yr_k, r, 0, 0))
            send(item(hc, left, 0), item(hc, left, 0), at(ys_k, r, 0, 2), at(yr_k, r, 0, 2), seq_1=right)
            arrive(item(hc, right, 0), at(ys_k, r, 0, 1), at(yr_k, r, 0, 1))
        else:
            arrive(item(hc, right, 1), at(ys_k, r, 1, 1), at(yr_k, r, 1, 1))
            send(item(hc, right, 1), item(hc, right, 1), at(ys_k, r, 1, 2), at(yr_k, r, 1, 2), seq_1=left)
            arrive(item(hc, left, 1), at(ys_k, r, 1, 0), at(yr_k, r, 1, 0))

    def core(r):
        hc = chunk[r]
        arrive(item(hc, across, 0), at(ys_k, r, 0, 2), at(yr_k, r, 0, 2))
        arrive(item(hc, across, 1), at(ys_k, r, 1, 2), at(yr_k, r, 1, 2))
        send(at(kv, c, hc), at(kv, c, hc), at(cs, VAL, r), at(cr, VAL, r), seq_2=mate)

    def core_in(r):
        hc = chunk[r]
        arrive(at(kv, mate, hc), at(cs, VAL, r), at(cr, VAL, r))

    def stacked(ref, g):
        return jnp.concatenate(
            [ref[:, pl.ds(pl.multiple_of(g * 512 + i * 128, 128), 128)] for i in range(4)], axis=0
        )

    def lanes(g):
        return pl.ds(pl.multiple_of(g * 128, 128), 128)

    def cross(r):
        hc = chunk[r]

        def one(g, _):
            keys = jnp.concatenate([im[i, hc, :, 0, :, lanes(g)].reshape(128, 128) for i in (0, 1)], axis=0)
            values = jnp.concatenate([im[i, hc, :, 1, :, lanes(g)].reshape(128, 128) for i in (0, 1)], axis=0)
            s = lax.dot_general(
                stacked(qx, g), keys, (((1,), (1,)), ((), ())), preferred_element_type=jnp.float32
            )
            at = lax.broadcasted_iota(jnp.int32, (1, 256), 1)
            slot = (((hc * 4 + (at % 128) // 32) * 2 + at // 128) * 32 + at % 32).astype(jnp.float32)
            bias = jnp.where((slot >= lo[:, :1]) & (slot < hi[:, :1]), 0.0, NEG)
            s = (s.reshape(4, 128, 256) * SCORE + bias[None]).reshape(512, 256)
            top = jnp.max(s, axis=1, keepdims=True)
            e = jnp.exp2(s - top)
            total = jnp.sum(e, axis=1, keepdims=True)
            weights = (e * jnp.where(top > 0.5 * NEG, 1.0 / total, 0.0)).astype(jnp.bfloat16)
            xc[g] += jnp.dot(weights, values, preferred_element_type=jnp.float32)
            grad = lax.dot_general(
                weights, stacked(ct, g), (((0,), (0,)), ((), ())), preferred_element_type=jnp.float32
            ).astype(jnp.bfloat16)
            for i in (0, 1):
                gs[r, i, :, :, lanes(g)] = grad[i * 128 : (i + 1) * 128].reshape(4, 32, 128)
            return 0

        lax.fori_loop(0, 2, one, 0)

    def attend(r):
        hc = chunk[r]

        def one(n, _):
            g, half_at = n // 2, n % 2
            keys = kv[half_at, hc, :, 0, :, lanes(g)].reshape(512, 128)
            values = kv[half_at, hc, :, 1, :, lanes(g)].reshape(512, 128)
            s = lax.dot_general(
                stacked(q, g), keys, (((1,), (1,)), ((), ())), preferred_element_type=jnp.float32
            )
            key_doc = jnp.concatenate([dg[half_at, hc, i] for i in range(4)], axis=1).astype(jnp.float32)
            at = lax.broadcasted_iota(jnp.int32, (128, 512), 1)
            key_pos = ((hc * 4 + at // 128) * 2 + half_at) * 128 + at % 128
            row_pos = own * 128 + lax.broadcasted_iota(jnp.int32, (128, 512), 0)
            bias = jnp.where((key_doc == qd[:, :1]) & (key_pos <= row_pos), 0.0, NEG)
            s = (s.reshape(4, 128, 512) * SCORE + bias[None]).reshape(512, 512)
            old = m_s[g][:, :1]
            top = jnp.maximum(old, jnp.max(s, axis=1, keepdims=True))
            e = jnp.exp2(s - top)
            fade = jnp.exp2(old - top)
            m_s[g] = jnp.broadcast_to(top, (512, 128))
            l_s[g] = l_s[g] * fade + jnp.broadcast_to(jnp.sum(e, axis=1, keepdims=True), (512, 128))
            acc[g] = acc[g] * fade + jnp.dot(e.astype(jnp.bfloat16), values, preferred_element_type=jnp.float32)
            return 0

        lax.fori_loop(0, 4, one, 0)

    def grad_out(r):
        for delta in range(1, 8):
            yy, cc = yc_of(delta)
            send(at(gs, r, cc, yy), at(gr, r, delta), at(gss, r, delta), at(gsr, r, delta), seq_1=yy, seq_2=cc)

    def grad_in(r):
        total = gs[r, c, y].astype(jnp.float32)
        for delta in range(1, 8):
            arrive(at(gr, r, delta), at(gss, r, delta), at(gsr, r, delta))
        for delta in range(1, 8):
            total += gr[r, delta].astype(jnp.float32)
        return total

    def owner_out(r):
        zs[r] = grad_in(r).astype(jnp.bfloat16)
        send(at(zs, r), at(zr, r), at(rss, r), at(rsr, r), seq_0=chunk[r])

    for way, where in ((0, up), (1, down)):
        send(doc(h, y), doc(h, y), at(zs_d, way), at(zr_d, way), seq_0=where)
        send(img(h, y), img(h, y), at(zs_i, way), at(zr_i, way), seq_0=where)
    on("up", lambda: z_half(0, 0, 0))
    on("low", lambda: z_half(1, 0, 1))
    y_first_small(0)
    for delta in range(1, 8):
        yy, cc = yc_of(delta)
        send(at(fs, yy * 2 + cc), at(gf, yc), at(fss, delta), at(fsr, delta), seq_1=yy, seq_2=cc)
    y_first(0, 0)
    y_first(0, 1)
    for copy in rest:
        copy.wait()

    y_second_small(0)
    core_small(0)
    y_second(0, 0)
    y_second(0, 1)
    core_small_in(0)
    cross(0)
    grad_out(0)
    core(0)

    arrive(doc(down, y), at(zs_d, 0), at(zr_d, 0))
    send(doc(down, y), doc(down, y), at(zs_d, 2), at(zr_d, 2), seq_0=up)
    arrive(img(down, y), at(zs_i, 0), at(zr_i, 0))
    send(img(down, y, 0), img(down, y, 0), at(zs_i, 2), at(zr_i, 2), seq_0=up)
    arrive(doc(up, y), at(zs_d, 1), at(zr_d, 1))
    arrive(img(up, y), at(zs_i, 1), at(zr_i, 1))
    send(img(up, y, 1), img(up, y, 1), at(zs_i, 3), at(zr_i, 3), seq_0=down)
    on("up", lambda: z_half(0, 1, 0), lambda: z_half(1, 0, 0), lambda: z_half(1, 1, 0))
    on("low", lambda: z_half(1, 1, 1))
    on("first", lambda: z_half(0, 0, 1), lambda: z_half(0, 1, 1))
    y_first_small(1)
    y_first_small(2)
    core_in(0)
    attend(0)
    y_second_small(1)
    y_second_small(2)
    core_small(1)
    core_small(2)
    vacc[...] = grad_in(0)
    core_small_in(1)
    cross(1)
    grad_out(1)
    core_small_in(2)
    cross(2)
    grad_out(2)

    arrive(doc(far, y), at(zs_d, 2), at(zr_d, 2))
    arrive(img(far, y, 0), at(zs_i, 2), at(zr_i, 2))
    arrive(img(far, y, 1), at(zs_i, 3), at(zr_i, 3))
    y_first_small(3)
    owner_out(1)
    owner_out(2)
    y_second_small(3)
    core_small(3)

    def keys_below():
        z_half_in(0, 0, 0)
        z_half_in(0, 1, 0)

    def values_above():
        z_half_in(1, 0, 1)
        z_half_in(1, 1, 1)
        send(item(up, y, 1), item(up, y, 1), at(zs_k, 1, 4), at(zr_k, 1, 4), seq_0=down)

    on(1, keys_below)
    on("mid", lambda: send(item(down, y, 0), item(down, y, 0), at(zs_k, 0, 4), at(zr_k, 0, 4), seq_0=up))
    on(1, lambda: y_first(1, 0))
    on("ends", values_above)
    on(2, lambda: y_first(2, 1))
    core_small_in(3)
    cross(3)
    grad_out(3)

    def keys_above():
        z_half_in(0, 0, 1)
        z_half_in(0, 1, 1)
        y_first(2, 0)

    def values_below():
        z_half_in(1, 0, 0)
        z_half_in(1, 1, 0)
        y_first(1, 1)

    on(1, lambda: y_second(1, 0))
    on(2, lambda: y_second(2, 1), keys_above)
    owner_out(3)
    on(1, values_below)
    on(2, lambda: y_second(2, 0), lambda: core(2))
    on(1, lambda: y_second(1, 1), lambda: core(1))
    on(2, lambda: core_in(2), lambda: attend(2))

    total = vacc[...]
    for r in (1, 2, 3):
        arrive(at(zr, r), at(rss, r), at(rsr, r))
    for r in (1, 2, 3):
        total += zr[r].astype(jnp.float32)
    vga[yc] = total.astype(jnp.bfloat16)
    for delta in range(1, 8):
        yy, cc = yc_of(delta)
        send(at(vga, yc), at(vga, yc), at(vss, delta), at(vsr, delta), seq_1=yy, seq_2=cc)
    on(1, lambda: core_in(1), lambda: attend(1))

    for delta in range(1, 8):
        yy, cc = yc_of(8 - delta)
        arrive(at(gf, yy * 2 + cc), at(fss, delta), at(fsr, delta))
        arrive(at(vga, yy * 2 + cc), at(vss, delta), at(vsr, delta))
    term = lax.dot_general(
        gf[...].reshape(256, 256), vga[...].reshape(256, 256), (((0,), (0,)), ((), ())),
        preferred_element_type=jnp.float32,
    )
    fw[...] = jnp.concatenate(
        [term[:, :128].reshape(32, 8, 128), term[:, 128:].reshape(32, 8, 128)], axis=1
    ).astype(jnp.bfloat16)
    for delta in sorted(range(1, 32), key=lambda d: abs(d - 16)):
        hh, bb = z_of(delta)
        send(at(fw, bb * 4 + hh), at(fr, delta), at(wss, delta), at(wsr, delta), seq_0=hh, dp=bb)

    def far_in():
        arrive(item(far, y, 0), at(zs_k, 0, 4), at(zr_k, 0, 4))
        y_first(3, 0)
        arrive(item(far, y, 1), at(zs_k, 1, 4), at(zr_k, 1, 4))
        y_first(3, 1)
        y_second(3, 0)
        y_second(3, 1)
        core(3)
        core_in(3)
        attend(3)

    on(3, far_in)

    for g in range(2):
        out = (acc[g] / l_s[g] + xc[g]).astype(jnp.bfloat16)
        for i in range(4):
            out_ref[0, :, (g * 4 + i) * 128 : (g * 4 + i + 1) * 128] = out[i * 128 : (i + 1) * 128]

    whole = fw[b * 4 + h].astype(jnp.float32)
    for delta in range(1, 32):
        arrive(at(fr, delta), at(wss, delta), at(wsr, delta))
    for delta in range(1, 32):
        whole += fr[delta].astype(jnp.float32)
    wg_ref[:, :128] = whole[:5]
    wg_ref[:, 128:] = whole[8:13]

    def drain(copies):
        for copy in copies:
            copy().wait_send()

    for key, copies in sends.items():
        if key == "all":
            drain(copies)
        elif copies:
            pl.when(conds[key])(functools.partial(drain, copies))


def on_device(*args):
    bf, f32, i32 = jnp.bfloat16, jnp.float32, jnp.int32
    any_space = pl.BlockSpec(memory_space=pl.ANY)
    vmem = pl.BlockSpec(memory_space=pltpu.VMEM)
    V, D = pltpu.VMEM, pltpu.SemaphoreType.DMA
    pairs = [(3,), (4,), (2, 5), (4, 3), (4, 4), (4, 2, 3), (3, 4), (8,), (4, 8), (4,), (8,), (32,)]
    return pl.pallas_call(
        kernel,
        out_shape=(
            jax.ShapeDtypeStruct((1, 128, 1024), bf),
            jax.ShapeDtypeStruct((5, 256), f32),
        ),
        in_specs=[any_space] * 9 + [vmem] * 2,
        out_specs=(vmem, vmem),
        scratch_shapes=[
            V((128, 1024), bf), V((128, 1024), bf), V((128, 1024), bf), V((32, 1280), bf), V((1280, 256), bf),
            V((2, 4, 4, 2, 128, 256), bf), V((2, 4, 4, 2, 32, 256), bf), V((2, 4, 4, 1, 128), i32),
            V((8, 32, 256), bf), V((8, 32, 256), bf),
            V((4, 2, 4, 32, 256), bf), V((4, 8, 32, 256), bf),
            V((4, 32, 256), bf), V((4, 32, 256), bf),
            V((8, 32, 256), bf), V((32, 16, 128), bf), V((32, 16, 128), bf),
            V((2, 512, 128), f32), V((2, 512, 128), f32), V((2, 512, 128), f32), V((2, 512, 128), f32),
            V((128, 128), f32), V((128, 128), f32), V((128, 128), f32), V((32, 256), f32),
            D((9,)),
        ]
        + [D(shape) for shape in pairs for _ in (0, 1)],
        compiler_params=pltpu.CompilerParams(
            collective_id=0, has_side_effects=True, vmem_limit_bytes=67043328
        ),
    )(*args)


def solution(mesh):
    split = Mesh(
        mesh.devices.reshape(mesh.shape["dp"], 4, 4, 2, mesh.shape["tensor"]),
        ("dp", "seq_0", "seq_1", "seq_2", "tensor"),
    )
    placed = (
        P("dp", SEQ, "tensor"),
        P("dp", SEQ, "tensor"),
        P("dp", SEQ, "tensor"),
        P("dp", SEQ),
        P("dp", SEQ, "tensor"),
        P("dp", SEQ, "tensor"),
        P("dp", SEQ, "tensor"),
        P("dp", SEQ, None),
        P(None, "tensor"),
        P("dp", None),
        P("dp", None),
    )
    return jax.shard_map(
        on_device,
        mesh=split,
        in_specs=placed,
        out_specs=(P("dp", SEQ, "tensor"), P(DP_SEQ, "tensor")),
        check_vma=False,
    )
```

```python
import functools
import math

import jax
import jax.numpy as jnp
from jax import lax
from jax.experimental import pallas as pl
from jax.experimental.pallas import tpu as pltpu
from jax.sharding import Mesh
from jax.sharding import PartitionSpec as P

HD = 128
TILE_TOK = 8
IMG_TOK = 32
SEQ = ("seq_0", "seq_1", "seq_2")
DP_SEQ = ("dp", "seq_0", "seq_1", "seq_2")
NEG = -1e30
MESH = pl.DeviceIdType.MESH
SCORE = HD**-0.5 * math.log2(math.e)

OFF = (0, 3, 1, 2)
DOC, KEY, VAL = 0, 1, 2


def kernel(
    q_hbm, k_hbm, v_hbm, docs_hbm, qx_hbm, ct_hbm, ik_hbm, f_hbm, w_hbm, tiles_ref, cite_ref,
    out_ref, wg_ref,
    q, qx, ct, feat, w,
    kv, im, dg, fs, gf, gs, gr, zs, zr, vga, fw, fr,
    m_s, l_s, acc, xc, qd, lo, hi, vacc,
    lsem,
    zs_d, zr_d, zs_i, zr_i, zs_k, zr_k,
    ys_d, yr_d, ys_i, yr_i, ys_k, yr_k,
    cs, cr, fss, fsr, gss, gsr, rss, rsr, vss, vsr, wss, wsr,
):
    b = lax.axis_index("dp")
    h = lax.axis_index("seq_0")
    y = lax.axis_index("seq_1")
    c = lax.axis_index("seq_2")
    yc = y * 2 + c
    own = h * 8 + yc
    pz = h * 8 + b
    up, down, far = (h + 1) % 4, (h + 3) % 4, (h + 2) % 4
    right, left, across = (y + 1) % 4, (y + 3) % 4, (y + 2) % 4
    chunk = (h, down, up, far)
    mate = 1 - c
    conds = {
        "all": None,
        "up": h <= 2,
        "low": h <= 1,
        "first": h == 0,
        "two": h == 2,
        "mid": (h == 1) | (h == 2),
        "ends": (h == 0) | (h == 3),
        1: h >= 1,
        2: h == 3,
        3: h >= 2,
    }
    sends = {key: [] for key in conds}
    now = ["all"]

    def on(key, *steps):
        def run():
            now[0] = key
            for step in steps:
                step()
            now[0] = "all"

        pl.when(conds[key])(run)

    def at(ref, *index):
        return ref, index

    def remote(*parts, **where):
        src, dst, ss, rs = (ref.at[index] for ref, index in parts)
        return pltpu.make_async_remote_copy(
            src_ref=src, dst_ref=dst, send_sem=ss, recv_sem=rs, device_id=where, device_id_type=MESH
        )

    def send(src, dst, ss, rs, **where):
        remote(src, dst, ss, rs, **where).start()
        sends[now[0]].append(lambda: remote(src, dst, ss, rs, **where))

    def arrive(dst, ss, rs):
        remote(dst, dst, ss, rs, seq_2=mate).wait_recv()

    def yc_of(delta):
        other = (yc + delta) % 8
        return other // 2, other % 2

    def z_of(delta):
        other = (pz + delta) % 32
        return other // 8, other % 8

    local = []

    def fetch(src, dst):
        copy = pltpu.make_async_copy(src, dst, lsem.at[len(local)])
        copy.start()
        local.append(copy)
        return copy

    got_f = fetch(f_hbm.at[0], feat)
    got_w = fetch(w_hbm, w)
    first = [
        fetch(docs_hbm, dg.at[c, h, y]),
        fetch(ik_hbm.at[0], im.at[c, h, y, 0]),
        fetch(k_hbm.at[0], kv.at[c, h, y, 0]),
        fetch(v_hbm.at[0], kv.at[c, h, y, 1]),
    ]
    rest = [fetch(q_hbm.at[0], q), fetch(qx_hbm.at[0], qx), fetch(ct_hbm.at[0], ct)]

    barrier = pltpu.get_barrier_semaphore()
    for where in (up, down):
        pl.semaphore_signal(barrier, inc=1, device_id={"seq_0": where}, device_id_type=MESH)
    for delta in range(1, 8):
        pl.semaphore_signal(barrier, inc=1, device_id={"dp": (b + delta) % 8}, device_id_type=MESH)
    for delta in range(1, 8):
        yy, cc = yc_of(delta)
        pl.semaphore_signal(barrier, inc=1, device_id={"seq_1": yy, "seq_2": cc}, device_id_type=MESH)

    for copy in first:
        copy.wait()
    pl.semaphore_wait(barrier, 16)

    def doc(hc, yy):
        return at(dg, c, hc, yy)

    def img(hc, yy, *part):
        return at(im, c, hc, yy, *part)

    def item(hc, yy, which):
        return at(kv, c, hc, yy, which)

    def half(hc, which, part):
        return at(kv, c, hc, y, which, pl.ds(part * 64, 64))

    def z_half(which, part, way):
        n = which * 2 + part
        where = up if way == 0 else down
        send(half(h, which, part), half(h, which, part), at(zs_k, way, n), at(zr_k, way, n), seq_0=where)

    def z_half_in(which, part, way):
        n = which * 2 + part
        hc = down if way == 0 else up
        arrive(half(hc, which, part), at(zs_k, way, n), at(zr_k, way, n))

    def y_first_small(r):
        hc = chunk[r]
        for way, where in ((0, right), (1, left)):
            send(doc(hc, y), doc(hc, y), at(ys_d, r, way), at(yr_d, r, way), seq_1=where)
            send(img(hc, y), img(hc, y), at(ys_i, r, way), at(yr_i, r, way), seq_1=where)

    def y_second_small(r):
        hc = chunk[r]
        arrive(doc(hc, left), at(ys_d, r, 0), at(yr_d, r, 0))
        send(doc(hc, left), doc(hc, left), at(ys_d, r, 2), at(yr_d, r, 2), seq_1=right)
        arrive(img(hc, left), at(ys_i, r, 0), at(yr_i, r, 0))
        send(img(hc, left, 0), img(hc, left, 0), at(ys_i, r, 2), at(yr_i, r, 2), seq_1=right)
        arrive(doc(hc, right), at(ys_d, r, 1), at(yr_d, r, 1))
        arrive(img(hc, right), at(ys_i, r, 1), at(yr_i, r, 1))
        send(img(hc, right, 1), img(hc, right, 1), at(ys_i, r, 3), at(yr_i, r, 3), seq_1=left)

    def core_small(r):
        hc = chunk[r]
        arrive(doc(hc, across), at(ys_d, r, 2), at(yr_d, r, 2))
        send(at(dg, c, hc), at(dg, c, hc), at(cs, DOC, r), at(cr, DOC, r), seq_2=mate)
        arrive(img(hc, across, 0), at(ys_i, r, 2), at(yr_i, r, 2))
        arrive(img(hc, across, 1), at(ys_i, r, 3), at(yr_i, r, 3))
        send(at(im, c, hc), at(im, c, hc), at(cs, KEY, r), at(cr, KEY, r), seq_2=mate)

    def core_small_in(r):
        hc = chunk[r]
        arrive(at(dg, mate, hc), at(cs, DOC, r), at(cr, DOC, r))
        arrive(at(im, mate, hc), at(cs, KEY, r), at(cr, KEY, r))

    def y_first(r, which):
        hc = chunk[r]
        for way, where in ((0, right), (1, left)):
            send(item(hc, y, which), item(hc, y, which), at(ys_k, r, which, way), at(yr_k, r, which, way), seq_1=where)

    def y_second(r, which):
        hc = chunk[r]
        if which == 0:
            arrive(item(hc, left, 0), at(ys_k, r, 0, 0), at(yr_k, r, 0, 0))
            send(item(hc, left, 0), item(hc, left, 0), at(ys_k, r, 0, 2), at(yr_k, r, 0, 2), seq_1=right)
            arrive(item(hc, right, 0), at(ys_k, r, 0, 1), at(yr_k, r, 0, 1))
        else:
            arrive(item(hc, right, 1), at(ys_k, r, 1, 1), at(yr_k, r, 1, 1))
            send(item(hc, right, 1), item(hc, right, 1), at(ys_k, r, 1, 2), at(yr_k, r, 1, 2), seq_1=left)
            arrive(item(hc, left, 1), at(ys_k, r, 1, 0), at(yr_k, r, 1, 0))

    def core(r):
        hc = chunk[r]
        arrive(item(hc, across, 0), at(ys_k, r, 0, 2), at(yr_k, r, 0, 2))
        arrive(item(hc, across, 1), at(ys_k, r, 1, 2), at(yr_k, r, 1, 2))
        send(at(kv, c, hc), at(kv, c, hc), at(cs, VAL, r), at(cr, VAL, r), seq_2=mate)

    def core_in(r):
        hc = chunk[r]
        arrive(at(kv, mate, hc), at(cs, VAL, r), at(cr, VAL, r))

    def stacked(ref, g):
        return jnp.concatenate(
            [ref[:, pl.ds(pl.multiple_of(g * 512 + i * 128, 128), 128)] for i in range(4)], axis=0
        )

    def lanes(g):
        return pl.ds(pl.multiple_of(g * 128, 128), 128)

    def cross(r):
        hc = chunk[r]

        def one(g, _):
            keys = jnp.concatenate([im[i, hc, :, 0, :, lanes(g)].reshape(128, 128) for i in (0, 1)], axis=0)
            values = jnp.concatenate([im[i, hc, :, 1, :, lanes(g)].reshape(128, 128) for i in (0, 1)], axis=0)
            s = lax.dot_general(
                stacked(qx, g), keys, (((1,), (1,)), ((), ())), preferred_element_type=jnp.float32
            )
            at = lax.broadcasted_iota(jnp.int32, (1, 256), 1)
            slot = (((hc * 4 + (at % 128) // 32) * 2 + at // 128) * 32 + at % 32).astype(jnp.float32)
            bias = jnp.where((slot >= lo[:, :1]) & (slot < hi[:, :1]), 0.0, NEG)
            s = (s.reshape(4, 128, 256) * SCORE + bias[None]).reshape(512, 256)
            top = jnp.max(s, axis=1, keepdims=True)
            e = jnp.exp2(s - top)
            total = jnp.sum(e, axis=1, keepdims=True)
            weights = (e * jnp.where(top > 0.5 * NEG, 1.0 / total, 0.0)).astype(jnp.bfloat16)
            xc[g] += jnp.dot(weights, values, preferred_element_type=jnp.float32)
            grad = lax.dot_general(
                weights, stacked(ct, g), (((0,), (0,)), ((), ())), preferred_element_type=jnp.float32
            ).astype(jnp.bfloat16)
            for i in (0, 1):
                gs[r, i, :, :, lanes(g)] = grad[i * 128 : (i + 1) * 128].reshape(4, 32, 128)
            return 0

        lax.fori_loop(0, 2, one, 0)

    def attend(r):
        hc = chunk[r]

        def one(n, _):
            g, half_at = n // 2, n % 2
            keys = kv[half_at, hc, :, 0, :, lanes(g)].reshape(512, 128)
            values = kv[half_at, hc, :, 1, :, lanes(g)].reshape(512, 128)
            s = lax.dot_general(
                stacked(q, g), keys, (((1,), (1,)), ((), ())), preferred_element_type=jnp.float32
            )
            key_doc = jnp.concatenate([dg[half_at, hc, i] for i in range(4)], axis=1).astype(jnp.float32)
            at = lax.broadcasted_iota(jnp.int32, (128, 512), 1)
            key_pos = ((hc * 4 + at // 128) * 2 + half_at) * 128 + at % 128
            row_pos = own * 128 + lax.broadcasted_iota(jnp.int32, (128, 512), 0)
            bias = jnp.where((key_doc == qd[:, :1]) & (key_pos <= row_pos), 0.0, NEG)
            s = (s.reshape(4, 128, 512) * SCORE + bias[None]).reshape(512, 512)
            old = m_s[g][:, :1]
            top = jnp.maximum(old, jnp.max(s, axis=1, keepdims=True))
            e = jnp.exp2(s - top)
            fade = jnp.exp2(old - top)
            m_s[g] = jnp.broadcast_to(top, (512, 128))
            l_s[g] = l_s[g] * fade + jnp.broadcast_to(jnp.sum(e, axis=1, keepdims=True), (512, 128))
            acc[g] = acc[g] * fade + jnp.dot(e.astype(jnp.bfloat16), values, preferred_element_type=jnp.float32)
            return 0

        lax.fori_loop(0, 4, one, 0)

    def grad_out(r):
        for delta in range(1, 8):
            yy, cc = yc_of(delta)
            send(at(gs, r, cc, yy), at(gr, r, delta), at(gss, r, delta), at(gsr, r, delta), seq_1=yy, seq_2=cc)

    def grad_in(r):
        total = gs[r, c, y].astype(jnp.float32)
        for delta in range(1, 8):
            arrive(at(gr, r, delta), at(gss, r, delta), at(gsr, r, delta))
        for delta in range(1, 8):
            total += gr[r, delta].astype(jnp.float32)
        return total

    def owner_out(r):
        zs[r] = grad_in(r).astype(jnp.bfloat16)
        send(at(zs, r), at(zr, r), at(rss, r), at(rsr, r), seq_0=chunk[r])

    for way, where in ((0, up), (1, down)):
        send(doc(h, y), doc(h, y), at(zs_d, way), at(zr_d, way), seq_0=where)
        send(img(h, y, 0), img(h, y, 0), at(zs_i, way), at(zr_i, way), seq_0=where)
    got_f.wait()
    got_w.wait()
    im[c, h, y, 1] = jnp.dot(feat[...], w[...], preferred_element_type=jnp.float32).astype(jnp.bfloat16)
    for way, where in ((0, up), (1, down)):
        send(img(h, y, 1), img(h, y, 1), at(zs_i, 4 + way), at(zr_i, 4 + way), seq_0=where)
    on("low", lambda: z_half(0, 0, 0), lambda: z_half(1, 0, 1))
    y_first_small(0)
    y_first(0, 0)
    y_first(0, 1)

    col = lax.broadcasted_iota(jnp.int32, (1, 256), 1)
    wanted = jnp.where(col % 8 < 5, (col // 8) * 40 + col % 8, -1000)
    vis_at = lax.broadcasted_iota(jnp.int32, (1280, 256), 0)

    def pick(partner, _):
        chosen = jnp.where(vis_at == wanted + partner * 5, 1.0, 0.0).astype(jnp.bfloat16)
        fs[partner] = jnp.dot(feat[...], chosen, preferred_element_type=jnp.float32).astype(jnp.bfloat16)
        return 0

    lax.fori_loop(0, 8, pick, 0)
    gf[yc] = fs[yc]

    for delta in range(1, 8):
        yy, cc = yc_of(delta)
        send(at(fs, yy * 2 + cc), at(gf, yc), at(fss, delta), at(fsr, delta), seq_1=yy, seq_2=cc)
    my_docs = jnp.broadcast_to(dg[c, h, y].astype(jnp.float32), (128, 128)).T
    qd[...] = my_docs
    number = lax.broadcasted_iota(jnp.int32, (128, 32), 1).astype(jnp.float32)
    cites = jnp.broadcast_to(cite_ref[...].astype(jnp.float32), (128, 32))
    counts = jnp.broadcast_to(tiles_ref[...].astype(jnp.float32), (128, 32))
    image = jnp.sum(jnp.where(number == my_docs[:, :32], cites, 0.0), axis=1, keepdims=True)
    tile_count = jnp.sum(jnp.where(number == image, counts, 0.0), axis=1, keepdims=True)
    lo[...] = jnp.broadcast_to(image * IMG_TOK, (128, 128))
    hi[...] = jnp.broadcast_to(image * IMG_TOK + tile_count * TILE_TOK, (128, 128))

    m_s[...] = jnp.full_like(m_s, NEG)
    l_s[...] = jnp.zeros_like(l_s)
    acc[...] = jnp.zeros_like(acc)
    xc[...] = jnp.zeros_like(xc)
    for copy in rest:
        copy.wait()

    y_second_small(0)
    core_small(0)
    y_second(0, 0)
    y_second(0, 1)
    core_small_in(0)
    cross(0)
    grad_out(0)
    core(0)

    arrive(doc(down, y), at(zs_d, 0), at(zr_d, 0))
    send(doc(down, y), doc(down, y), at(zs_d, 2), at(zr_d, 2), seq_0=up)
    arrive(img(down, y, 0), at(zs_i, 0), at(zr_i, 0))
    send(img(down, y, 0), img(down, y, 0), at(zs_i, 2), at(zr_i, 2), seq_0=up)
    arrive(doc(up, y), at(zs_d, 1), at(zr_d, 1))
    arrive(img(up, y, 0), at(zs_i, 1), at(zr_i, 1))
    arrive(img(up, y, 1), at(zs_i, 5), at(zr_i, 5))
    send(img(up, y, 1), img(up, y, 1), at(zs_i, 3), at(zr_i, 3), seq_0=down)
    arrive(img(down, y, 1), at(zs_i, 4), at(zr_i, 4))
    on("two", lambda: z_half(0, 0, 0))
    on("up", lambda: z_half(0, 1, 0), lambda: z_half(1, 0, 0), lambda: z_half(1, 1, 0))
    on("low", lambda: z_half(1, 1, 1))
    on("first", lambda: z_half(0, 0, 1), lambda: z_half(0, 1, 1))
    y_first_small(1)
    y_first_small(2)
    core_in(0)
    attend(0)
    y_second_small(1)
    y_second_small(2)
    core_small(1)
    core_small(2)
    vacc[...] = grad_in(0)
    core_small_in(1)
    cross(1)
    grad_out(1)
    core_small_in(2)
    cross(2)
    grad_out(2)

    arrive(doc(far, y), at(zs_d, 2), at(zr_d, 2))
    arrive(img(far, y, 0), at(zs_i, 2), at(zr_i, 2))
    arrive(img(far, y, 1), at(zs_i, 3), at(zr_i, 3))
    y_first_small(3)
    owner_out(1)
    owner_out(2)
    y_second_small(3)
    core_small(3)

    def keys_below():
        z_half_in(0, 0, 0)
        z_half_in(0, 1, 0)

    def values_above():
        z_half_in(1, 0, 1)
        z_half_in(1, 1, 1)
        send(item(up, y, 1), item(up, y, 1), at(zs_k, 1, 4), at(zr_k, 1, 4), seq_0=down)

    on(
        "mid",
        keys_below,
        lambda: send(item(down, y, 0), item(down, y, 0), at(zs_k, 0, 4), at(zr_k, 0, 4), seq_0=up),
        lambda: y_first(1, 0),
    )
    on("ends", values_above)
    on(2, lambda: y_first(2, 1))
    core_small_in(3)
    cross(3)
    grad_out(3)

    def keys_above():
        z_half_in(0, 0, 1)
        z_half_in(0, 1, 1)
        y_first(2, 0)

    def values_below():
        z_half_in(1, 0, 0)
        z_half_in(1, 1, 0)
        y_first(1, 1)

    on("mid", lambda: y_second(1, 0))
    on(2, lambda: y_second(2, 1))
    owner_out(3)
    on(2, keys_above, lambda: y_second(2, 0), lambda: core(2), keys_below, lambda: y_first(1, 0), lambda: y_second(1, 0))
    on(1, values_below, lambda: y_second(1, 1), lambda: core(1))

    total = vacc[...]
    for r in (1, 2, 3):
        arrive(at(zr, r), at(rss, r), at(rsr, r))
    for r in (1, 2, 3):
        total += zr[r].astype(jnp.float32)
    vga[yc] = total.astype(jnp.bfloat16)
    for delta in range(1, 8):
        yy, cc = yc_of(delta)
        send(at(vga, yc), at(vga, yc), at(vss, delta), at(vsr, delta), seq_1=yy, seq_2=cc)
    on(2, lambda: core_in(2), lambda: attend(2))

    for delta in range(1, 8):
        yy, cc = yc_of(8 - delta)
        arrive(at(gf, yy * 2 + cc), at(fss, delta), at(fsr, delta))
        arrive(at(vga, yy * 2 + cc), at(vss, delta), at(vsr, delta))
    term = lax.dot_general(
        gf[...].reshape(256, 256), vga[...].reshape(256, 256), (((0,), (0,)), ((), ())),
        preferred_element_type=jnp.float32,
    )
    fw[...] = jnp.concatenate(
        [term[:, :128].reshape(32, 8, 128), term[:, 128:].reshape(32, 8, 128)], axis=1
    ).astype(jnp.bfloat16)
    for delta in sorted(range(1, 32), key=lambda d: abs(d - 16)):
        hh, bb = z_of(delta)
        send(at(fw, bb * 4 + hh), at(fr, delta), at(wss, delta), at(wsr, delta), seq_0=hh, dp=bb)
    on(1, lambda: core_in(1), lambda: attend(1))

    def far_in():
        arrive(item(far, y, 0), at(zs_k, 0, 4), at(zr_k, 0, 4))
        y_first(3, 0)
        arrive(item(far, y, 1), at(zs_k, 1, 4), at(zr_k, 1, 4))
        y_first(3, 1)
        y_second(3, 0)
        y_second(3, 1)
        core(3)
        core_in(3)
        attend(3)

    on(3, far_in)

    for g in range(2):
        out = (acc[g] / l_s[g] + xc[g]).astype(jnp.bfloat16)
        for i in range(4):
            out_ref[0, :, (g * 4 + i) * 128 : (g * 4 + i + 1) * 128] = out[i * 128 : (i + 1) * 128]

    whole = fw[b * 4 + h].astype(jnp.float32)
    for delta in range(1, 32):
        arrive(at(fr, delta), at(wss, delta), at(wsr, delta))
    for delta in range(1, 32):
        whole += fr[delta].astype(jnp.float32)
    wg_ref[:, :128] = whole[:5]
    wg_ref[:, 128:] = whole[8:13]

    def drain(copies):
        for copy in copies:
            copy().wait_send()

    for key, copies in sends.items():
        if key == "all":
            drain(copies)
        elif copies:
            pl.when(conds[key])(functools.partial(drain, copies))


def on_device(*args):
    bf, f32, i32 = jnp.bfloat16, jnp.float32, jnp.int32
    any_space = pl.BlockSpec(memory_space=pl.ANY)
    vmem = pl.BlockSpec(memory_space=pltpu.VMEM)
    V, D = pltpu.VMEM, pltpu.SemaphoreType.DMA
    pairs = [(3,), (6,), (2, 5), (4, 3), (4, 4), (4, 2, 3), (3, 4), (8,), (4, 8), (4,), (8,), (32,)]
    return pl.pallas_call(
        kernel,
        out_shape=(
            jax.ShapeDtypeStruct((1, 128, 1024), bf),
            jax.ShapeDtypeStruct((5, 256), f32),
        ),
        in_specs=[any_space] * 9 + [vmem] * 2,
        out_specs=(vmem, vmem),
        scratch_shapes=[
            V((128, 1024), bf), V((128, 1024), bf), V((128, 1024), bf), V((32, 1280), bf), V((1280, 256), bf),
            V((2, 4, 4, 2, 128, 256), bf), V((2, 4, 4, 2, 32, 256), bf), V((2, 4, 4, 1, 128), i32),
            V((8, 32, 256), bf), V((8, 32, 256), bf),
            V((4, 2, 4, 32, 256), bf), V((4, 8, 32, 256), bf),
            V((4, 32, 256), bf), V((4, 32, 256), bf),
            V((8, 32, 256), bf), V((32, 16, 128), bf), V((32, 16, 128), bf),
            V((2, 512, 128), f32), V((2, 512, 128), f32), V((2, 512, 128), f32), V((2, 512, 128), f32),
            V((128, 128), f32), V((128, 128), f32), V((128, 128), f32), V((32, 256), f32),
            D((9,)),
        ]
        + [D(shape) for shape in pairs for _ in (0, 1)],
        compiler_params=pltpu.CompilerParams(
            collective_id=0, has_side_effects=True, vmem_limit_bytes=67043328
        ),
    )(*args)


def solution(mesh):
    split = Mesh(
        mesh.devices.reshape(mesh.shape["dp"], 4, 4, 2, mesh.shape["tensor"]),
        ("dp", "seq_0", "seq_1", "seq_2", "tensor"),
    )
    placed = (
        P("dp", SEQ, "tensor"),
        P("dp", SEQ, "tensor"),
        P("dp", SEQ, "tensor"),
        P("dp", SEQ),
        P("dp", SEQ, "tensor"),
        P("dp", SEQ, "tensor"),
        P("dp", SEQ, "tensor"),
        P("dp", SEQ, None),
        P(None, "tensor"),
        P("dp", None),
        P("dp", None),
    )
    return jax.shard_map(
        on_device,
        mesh=split,
        in_specs=placed,
        out_specs=(P("dp", SEQ, "tensor"), P(DP_SEQ, "tensor")),
        check_vma=False,
    )
```

```python
import functools
import math

import jax
import jax.numpy as jnp
from jax import lax
from jax.experimental import pallas as pl
from jax.experimental.pallas import tpu as pltpu
from jax.sharding import Mesh
from jax.sharding import PartitionSpec as P

HD = 128
TILE_TOK = 8
IMG_TOK = 32
SEQ = ("seq_0", "seq_1", "seq_2")
DP_SEQ = ("dp", "seq_0", "seq_1", "seq_2")
NEG = -1e30
MESH = pl.DeviceIdType.MESH
SCORE = HD**-0.5 * math.log2(math.e)

OFF = (0, 3, 1, 2)
DOC, KEY, VAL = 0, 1, 2


def kernel(
    q_hbm, k_hbm, v_hbm, docs_hbm, qx_hbm, ct_hbm, ik_hbm, f_hbm, w_hbm, tiles_ref, cite_ref,
    out_ref, wg_ref,
    q, qx, ct, feat, w,
    kv, im, dg, fs, gf, gs, gr, zs, zr, vga, fw, fr,
    m_s, l_s, acc, xc, qd, lo, hi, vacc,
    lsem,
    zs_d, zr_d, zs_i, zr_i, zs_k, zr_k,
    ys_d, yr_d, ys_i, yr_i, ys_k, yr_k,
    cs, cr, fss, fsr, gss, gsr, rss, rsr, vss, vsr, wss, wsr,
):
    b = lax.axis_index("dp")
    h = lax.axis_index("seq_0")
    y = lax.axis_index("seq_1")
    c = lax.axis_index("seq_2")
    yc = y * 2 + c
    own = h * 8 + yc
    pz = h * 8 + b
    up, down, far = (h + 1) % 4, (h + 3) % 4, (h + 2) % 4
    right, left, across = (y + 1) % 4, (y + 3) % 4, (y + 2) % 4
    chunk = (h, down, up, far)
    mate = 1 - c
    conds = {
        "all": None,
        "up": h <= 2,
        "low": h <= 1,
        "first": h == 0,
        "mid": (h == 1) | (h == 2),
        "ends": (h == 0) | (h == 3),
        1: h >= 1,
        2: h == 3,
        3: h >= 2,
    }
    sends = {key: [] for key in conds}
    now = ["all"]

    def on(key, *steps):
        def run():
            now[0] = key
            for step in steps:
                step()
            now[0] = "all"

        pl.when(conds[key])(run)

    def at(ref, *index):
        return ref, index

    def remote(*parts, **where):
        src, dst, ss, rs = (ref.at[index] for ref, index in parts)
        return pltpu.make_async_remote_copy(
            src_ref=src, dst_ref=dst, send_sem=ss, recv_sem=rs, device_id=where, device_id_type=MESH
        )

    def send(src, dst, ss, rs, **where):
        remote(src, dst, ss, rs, **where).start()
        sends[now[0]].append(lambda: remote(src, dst, ss, rs, **where))

    def arrive(dst, ss, rs):
        remote(dst, dst, ss, rs, seq_2=mate).wait_recv()

    def yc_of(delta):
        other = (yc + delta) % 8
        return other // 2, other % 2

    def z_of(delta):
        other = (pz + delta) % 32
        return other // 8, other % 8

    local = []

    def fetch(src, dst):
        copy = pltpu.make_async_copy(src, dst, lsem.at[len(local)])
        copy.start()
        local.append(copy)
        return copy

    got_f = fetch(f_hbm.at[0], feat)
    got_w = fetch(w_hbm, w)
    first = [
        fetch(docs_hbm, dg.at[c, h, y]),
        fetch(ik_hbm.at[0], im.at[c, h, y, 0]),
        fetch(k_hbm.at[0], kv.at[c, h, y, 0]),
        fetch(v_hbm.at[0], kv.at[c, h, y, 1]),
    ]
    rest = [fetch(q_hbm.at[0], q), fetch(qx_hbm.at[0], qx), fetch(ct_hbm.at[0], ct)]

    barrier = pltpu.get_barrier_semaphore()
    for where in (up, down):
        pl.semaphore_signal(barrier, inc=1, device_id={"seq_0": where}, device_id_type=MESH)
    for delta in range(1, 8):
        pl.semaphore_signal(barrier, inc=1, device_id={"dp": (b + delta) % 8}, device_id_type=MESH)
    for delta in range(1, 8):
        yy, cc = yc_of(delta)
        pl.semaphore_signal(barrier, inc=1, device_id={"seq_1": yy, "seq_2": cc}, device_id_type=MESH)

    got_f.wait()
    got_w.wait()
    im[c, h, y, 1] = jnp.dot(feat[...], w[...], preferred_element_type=jnp.float32).astype(jnp.bfloat16)

    col = lax.broadcasted_iota(jnp.int32, (1, 256), 1)
    wanted = jnp.where(col % 8 < 5, (col // 8) * 40 + col % 8, -1000)
    vis_at = lax.broadcasted_iota(jnp.int32, (1280, 256), 0)

    def pick(partner, _):
        chosen = jnp.where(vis_at == wanted + partner * 5, 1.0, 0.0).astype(jnp.bfloat16)
        fs[partner] = jnp.dot(feat[...], chosen, preferred_element_type=jnp.float32).astype(jnp.bfloat16)
        return 0

    lax.fori_loop(0, 8, pick, 0)
    gf[yc] = fs[yc]

    m_s[...] = jnp.full_like(m_s, NEG)
    l_s[...] = jnp.zeros_like(l_s)
    acc[...] = jnp.zeros_like(acc)
    xc[...] = jnp.zeros_like(xc)

    for copy in first:
        copy.wait()
    my_docs = jnp.broadcast_to(dg[c, h, y].astype(jnp.float32), (128, 128)).T
    qd[...] = my_docs
    number = lax.broadcasted_iota(jnp.int32, (128, 32), 1).astype(jnp.float32)
    cites = jnp.broadcast_to(cite_ref[...].astype(jnp.float32), (128, 32))
    counts = jnp.broadcast_to(tiles_ref[...].astype(jnp.float32), (128, 32))
    image = jnp.sum(jnp.where(number == my_docs[:, :32], cites, 0.0), axis=1, keepdims=True)
    tile_count = jnp.sum(jnp.where(number == image, counts, 0.0), axis=1, keepdims=True)
    lo[...] = jnp.broadcast_to(image * IMG_TOK, (128, 128))
    hi[...] = jnp.broadcast_to(image * IMG_TOK + tile_count * TILE_TOK, (128, 128))

    pl.semaphore_wait(barrier, 16)

    def doc(hc, yy):
        return at(dg, c, hc, yy)

    def img(hc, yy, *part):
        return at(im, c, hc, yy, *part)

    def item(hc, yy, which):
        return at(kv, c, hc, yy, which)

    def half(hc, which, part):
        return at(kv, c, hc, y, which, pl.ds(part * 64, 64))

    def z_half(which, part, way):
        n = which * 2 + part
        where = up if way == 0 else down
        send(half(h, which, part), half(h, which, part), at(zs_k, way, n), at(zr_k, way, n), seq_0=where)

    def z_half_in(which, part, way):
        n = which * 2 + part
        hc = down if way == 0 else up
        arrive(half(hc, which, part), at(zs_k, way, n), at(zr_k, way, n))

    def y_first_small(r):
        hc = chunk[r]
        for way, where in ((0, right), (1, left)):
            send(doc(hc, y), doc(hc, y), at(ys_d, r, way), at(yr_d, r, way), seq_1=where)
            send(img(hc, y), img(hc, y), at(ys_i, r, way), at(yr_i, r, way), seq_1=where)

    def y_second_small(r):
        hc = chunk[r]
        arrive(doc(hc, left), at(ys_d, r, 0), at(yr_d, r, 0))
        send(doc(hc, left), doc(hc, left), at(ys_d, r, 2), at(yr_d, r, 2), seq_1=right)
        arrive(img(hc, left), at(ys_i, r, 0), at(yr_i, r, 0))
        send(img(hc, left, 0), img(hc, left, 0), at(ys_i, r, 2), at(yr_i, r, 2), seq_1=right)
        arrive(doc(hc, right), at(ys_d, r, 1), at(yr_d, r, 1))
        arrive(img(hc, right), at(ys_i, r, 1), at(yr_i, r, 1))
        send(img(hc, right, 1), img(hc, right, 1), at(ys_i, r, 3), at(yr_i, r, 3), seq_1=left)

    def core_small(r):
        hc = chunk[r]
        arrive(doc(hc, across), at(ys_d, r, 2), at(yr_d, r, 2))
        send(at(dg, c, hc), at(dg, c, hc), at(cs, DOC, r), at(cr, DOC, r), seq_2=mate)
        arrive(img(hc, across, 0), at(ys_i, r, 2), at(yr_i, r, 2))
        arrive(img(hc, across, 1), at(ys_i, r, 3), at(yr_i, r, 3))
        send(at(im, c, hc), at(im, c, hc), at(cs, KEY, r), at(cr, KEY, r), seq_2=mate)

    def core_small_in(r):
        hc = chunk[r]
        arrive(at(dg, mate, hc), at(cs, DOC, r), at(cr, DOC, r))
        arrive(at(im, mate, hc), at(cs, KEY, r), at(cr, KEY, r))

    def y_first(r, which):
        hc = chunk[r]
        for way, where in ((0, right), (1, left)):
            send(item(hc, y, which), item(hc, y, which), at(ys_k, r, which, way), at(yr_k, r, which, way), seq_1=where)

    def y_second(r, which):
        hc = chunk[r]
        if which == 0:
            arrive(item(hc, left, 0), at(ys_k, r, 0, 0), at(yr_k, r, 0, 0))
            send(item(hc, left, 0), item(hc, left, 0), at(ys_k, r, 0, 2), at(yr_k, r, 0, 2), seq_1=right)
            arrive(item(hc, right, 0), at(ys_k, r, 0, 1), at(yr_k, r, 0, 1))
        else:
            arrive(item(hc, right, 1), at(ys_k, r, 1, 1), at(yr_k, r, 1, 1))
            send(item(hc, right, 1), item(hc, right, 1), at(ys_k, r, 1, 2), at(yr_k, r, 1, 2), seq_1=left)
            arrive(item(hc, left, 1), at(ys_k, r, 1, 0), at(yr_k, r, 1, 0))

    def core(r):
        hc = chunk[r]
        arrive(item(hc, across, 0), at(ys_k, r, 0, 2), at(yr_k, r, 0, 2))
        arrive(item(hc, across, 1), at(ys_k, r, 1, 2), at(yr_k, r, 1, 2))
        send(at(kv, c, hc), at(kv, c, hc), at(cs, VAL, r), at(cr, VAL, r), seq_2=mate)

    def core_in(r):
        hc = chunk[r]
        arrive(at(kv, mate, hc), at(cs, VAL, r), at(cr, VAL, r))

    def stacked(ref, g):
        return jnp.concatenate(
            [ref[:, pl.ds(pl.multiple_of(g * 512 + i * 128, 128), 128)] for i in range(4)], axis=0
        )

    def lanes(g):
        return pl.ds(pl.multiple_of(g * 128, 128), 128)

    def cross(r):
        hc = chunk[r]

        def one(g, _):
            keys = jnp.concatenate([im[i, hc, :, 0, :, lanes(g)].reshape(128, 128) for i in (0, 1)], axis=0)
            values = jnp.concatenate([im[i, hc, :, 1, :, lanes(g)].reshape(128, 128) for i in (0, 1)], axis=0)
            s = lax.dot_general(
                stacked(qx, g), keys, (((1,), (1,)), ((), ())), preferred_element_type=jnp.float32
            )
            at = lax.broadcasted_iota(jnp.int32, (1, 256), 1)
            slot = (((hc * 4 + (at % 128) // 32) * 2 + at // 128) * 32 + at % 32).astype(jnp.float32)
            bias = jnp.where((slot >= lo[:, :1]) & (slot < hi[:, :1]), 0.0, NEG)
            s = (s.reshape(4, 128, 256) * SCORE + bias[None]).reshape(512, 256)
            top = jnp.max(s, axis=1, keepdims=True)
            e = jnp.exp2(s - top)
            total = jnp.sum(e, axis=1, keepdims=True)
            weights = (e * jnp.where(top > 0.5 * NEG, 1.0 / total, 0.0)).astype(jnp.bfloat16)
            xc[g] += jnp.dot(weights, values, preferred_element_type=jnp.float32)
            grad = lax.dot_general(
                weights, stacked(ct, g), (((0,), (0,)), ((), ())), preferred_element_type=jnp.float32
            ).astype(jnp.bfloat16)
            for i in (0, 1):
                gs[r, i, :, :, lanes(g)] = grad[i * 128 : (i + 1) * 128].reshape(4, 32, 128)
            return 0

        lax.fori_loop(0, 2, one, 0)

    def attend(r):
        hc = chunk[r]

        def one(n, _):
            g, half_at = n // 2, n % 2
            keys = kv[half_at, hc, :, 0, :, lanes(g)].reshape(512, 128)
            values = kv[half_at, hc, :, 1, :, lanes(g)].reshape(512, 128)
            s = lax.dot_general(
                stacked(q, g), keys, (((1,), (1,)), ((), ())), preferred_element_type=jnp.float32
            )
            key_doc = jnp.concatenate([dg[half_at, hc, i] for i in range(4)], axis=1).astype(jnp.float32)
            at = lax.broadcasted_iota(jnp.int32, (128, 512), 1)
            key_pos = ((hc * 4 + at // 128) * 2 + half_at) * 128 + at % 128
            row_pos = own * 128 + lax.broadcasted_iota(jnp.int32, (128, 512), 0)
            bias = jnp.where((key_doc == qd[:, :1]) & (key_pos <= row_pos), 0.0, NEG)
            s = (s.reshape(4, 128, 512) * SCORE + bias[None]).reshape(512, 512)
            old = m_s[g][:, :1]
            top = jnp.maximum(old, jnp.max(s, axis=1, keepdims=True))
            e = jnp.exp2(s - top)
            fade = jnp.exp2(old - top)
            m_s[g] = jnp.broadcast_to(top, (512, 128))
            l_s[g] = l_s[g] * fade + jnp.broadcast_to(jnp.sum(e, axis=1, keepdims=True), (512, 128))
            acc[g] = acc[g] * fade + jnp.dot(e.astype(jnp.bfloat16), values, preferred_element_type=jnp.float32)
            return 0

        lax.fori_loop(0, 4, one, 0)

    def grad_out(r):
        for delta in range(1, 8):
            yy, cc = yc_of(delta)
            send(at(gs, r, cc, yy), at(gr, r, delta), at(gss, r, delta), at(gsr, r, delta), seq_1=yy, seq_2=cc)

    def grad_in(r):
        total = gs[r, c, y].astype(jnp.float32)
        for delta in range(1, 8):
            arrive(at(gr, r, delta), at(gss, r, delta), at(gsr, r, delta))
        for delta in range(1, 8):
            total += gr[r, delta].astype(jnp.float32)
        return total

    def owner_out(r):
        zs[r] = grad_in(r).astype(jnp.bfloat16)
        send(at(zs, r), at(zr, r), at(rss, r), at(rsr, r), seq_0=chunk[r])

    for way, where in ((0, up), (1, down)):
        send(doc(h, y), doc(h, y), at(zs_d, way), at(zr_d, way), seq_0=where)
        send(img(h, y), img(h, y), at(zs_i, way), at(zr_i, way), seq_0=where)
    on("up", lambda: z_half(0, 0, 0))
    on("low", lambda: z_half(1, 0, 1))
    y_first_small(0)
    for delta in range(1, 8):
        yy, cc = yc_of(delta)
        send(at(fs, yy * 2 + cc), at(gf, yc), at(fss, delta), at(fsr, delta), seq_1=yy, seq_2=cc)
    y_first(0, 0)
    y_first(0, 1)
    for copy in rest:
        copy.wait()

    y_second_small(0)
    core_small(0)
    y_second(0, 0)
    y_second(0, 1)
    core_small_in(0)
    cross(0)
    grad_out(0)
    core(0)

    arrive(doc(down, y), at(zs_d, 0), at(zr_d, 0))
    send(doc(down, y), doc(down, y), at(zs_d, 2), at(zr_d, 2), seq_0=up)
    arrive(img(down, y), at(zs_i, 0), at(zr_i, 0))
    send(img(down, y, 0), img(down, y, 0), at(zs_i, 2), at(zr_i, 2), seq_0=up)
    arrive(doc(up, y), at(zs_d, 1), at(zr_d, 1))
    arrive(img(up, y), at(zs_i, 1), at(zr_i, 1))
    send(img(up, y, 1), img(up, y, 1), at(zs_i, 3), at(zr_i, 3), seq_0=down)
    on("up", lambda: z_half(0, 1, 0), lambda: z_half(1, 0, 0), lambda: z_half(1, 1, 0))
    on("low", lambda: z_half(1, 1, 1))
    on("first", lambda: z_half(0, 0, 1), lambda: z_half(0, 1, 1))
    y_first_small(1)
    y_first_small(2)
    core_in(0)
    attend(0)
    y_second_small(1)
    y_second_small(2)
    core_small(1)
    core_small(2)
    vacc[...] = grad_in(0)
    core_small_in(1)
    cross(1)
    grad_out(1)
    core_small_in(2)
    cross(2)
    grad_out(2)

    arrive(doc(far, y), at(zs_d, 2), at(zr_d, 2))
    arrive(img(far, y, 0), at(zs_i, 2), at(zr_i, 2))
    arrive(img(far, y, 1), at(zs_i, 3), at(zr_i, 3))
    y_first_small(3)
    owner_out(1)
    owner_out(2)
    y_second_small(3)
    core_small(3)

    def keys_below():
        z_half_in(0, 0, 0)
        z_half_in(0, 1, 0)

    def values_above():
        z_half_in(1, 0, 1)
        z_half_in(1, 1, 1)
        send(item(up, y, 1), item(up, y, 1), at(zs_k, 1, 4), at(zr_k, 1, 4), seq_0=down)

    on(1, keys_below)
    on("mid", lambda: send(item(down, y, 0), item(down, y, 0), at(zs_k, 0, 4), at(zr_k, 0, 4), seq_0=up))
    on(1, lambda: y_first(1, 0))
    on("ends", values_above)
    on(2, lambda: y_first(2, 1))
    core_small_in(3)
    cross(3)
    grad_out(3)

    def keys_above():
        z_half_in(0, 0, 1)
        z_half_in(0, 1, 1)
        y_first(2, 0)

    def values_below():
        z_half_in(1, 0, 0)
        z_half_in(1, 1, 0)
        y_first(1, 1)

    on(1, lambda: y_second(1, 0))
    on(2, lambda: y_second(2, 1))
    owner_out(3)
    on(1, values_below)

    total = vacc[...]
    for r in (1, 2, 3):
        arrive(at(zr, r), at(rss, r), at(rsr, r))
    for r in (1, 2, 3):
        total += zr[r].astype(jnp.float32)
    vga[yc] = total.astype(jnp.bfloat16)
    for delta in range(1, 8):
        yy, cc = yc_of(delta)
        send(at(vga, yc), at(vga, yc), at(vss, delta), at(vsr, delta), seq_1=yy, seq_2=cc)
    on(2, keys_above)
    on(1, lambda: y_second(1, 1), lambda: core(1))
    on(2, lambda: y_second(2, 0), lambda: core(2))

    for delta in range(1, 8):
        yy, cc = yc_of(8 - delta)
        arrive(at(gf, yy * 2 + cc), at(fss, delta), at(fsr, delta))
        arrive(at(vga, yy * 2 + cc), at(vss, delta), at(vsr, delta))
    term = lax.dot_general(
        gf[...].reshape(256, 256), vga[...].reshape(256, 256), (((0,), (0,)), ((), ())),
        preferred_element_type=jnp.float32,
    )
    fw[...] = jnp.concatenate(
        [term[:, :128].reshape(32, 8, 128), term[:, 128:].reshape(32, 8, 128)], axis=1
    ).astype(jnp.bfloat16)
    for delta in sorted(range(1, 32), key=lambda d: abs(d - 16)):
        hh, bb = z_of(delta)
        send(at(fw, bb * 4 + hh), at(fr, delta), at(wss, delta), at(wsr, delta), seq_0=hh, dp=bb)
    on(1, lambda: core_in(1), lambda: attend(1))
    on(2, lambda: core_in(2), lambda: attend(2))

    def far_in():
        arrive(item(far, y, 0), at(zs_k, 0, 4), at(zr_k, 0, 4))
        y_first(3, 0)
        arrive(item(far, y, 1), at(zs_k, 1, 4), at(zr_k, 1, 4))
        y_first(3, 1)
        y_second(3, 0)
        y_second(3, 1)
        core(3)
        core_in(3)
        attend(3)

    on(3, far_in)

    for g in range(2):
        out = (acc[g] / l_s[g] + xc[g]).astype(jnp.bfloat16)
        for i in range(4):
            out_ref[0, :, (g * 4 + i) * 128 : (g * 4 + i + 1) * 128] = out[i * 128 : (i + 1) * 128]

    whole = fw[b * 4 + h].astype(jnp.float32)
    for delta in range(1, 32):
        arrive(at(fr, delta), at(wss, delta), at(wsr, delta))
    for delta in range(1, 32):
        whole += fr[delta].astype(jnp.float32)
    wg_ref[:, :128] = whole[:5]
    wg_ref[:, 128:] = whole[8:13]

    def drain(copies):
        for copy in copies:
            copy().wait_send()

    for key, copies in sends.items():
        if key == "all":
            drain(copies)
        elif copies:
            pl.when(conds[key])(functools.partial(drain, copies))


def on_device(*args):
    bf, f32, i32 = jnp.bfloat16, jnp.float32, jnp.int32
    any_space = pl.BlockSpec(memory_space=pl.ANY)
    vmem = pl.BlockSpec(memory_space=pltpu.VMEM)
    V, D = pltpu.VMEM, pltpu.SemaphoreType.DMA
    pairs = [(3,), (4,), (2, 5), (4, 3), (4, 4), (4, 2, 3), (3, 4), (8,), (4, 8), (4,), (8,), (32,)]
    return pl.pallas_call(
        kernel,
        out_shape=(
            jax.ShapeDtypeStruct((1, 128, 1024), bf),
            jax.ShapeDtypeStruct((5, 256), f32),
        ),
        in_specs=[any_space] * 9 + [vmem] * 2,
        out_specs=(vmem, vmem),
        scratch_shapes=[
            V((128, 1024), bf), V((128, 1024), bf), V((128, 1024), bf), V((32, 1280), bf), V((1280, 256), bf),
            V((2, 4, 4, 2, 128, 256), bf), V((2, 4, 4, 2, 32, 256), bf), V((2, 4, 4, 1, 128), i32),
            V((8, 32, 256), bf), V((8, 32, 256), bf),
            V((4, 2, 4, 32, 256), bf), V((4, 8, 32, 256), bf),
            V((4, 32, 256), bf), V((4, 32, 256), bf),
            V((8, 32, 256), bf), V((32, 16, 128), bf), V((32, 16, 128), bf),
            V((2, 512, 128), f32), V((2, 512, 128), f32), V((2, 512, 128), f32), V((2, 512, 128), f32),
            V((128, 128), f32), V((128, 128), f32), V((128, 128), f32), V((32, 256), f32),
            D((9,)),
        ]
        + [D(shape) for shape in pairs for _ in (0, 1)],
        compiler_params=pltpu.CompilerParams(
            collective_id=0, has_side_effects=True, vmem_limit_bytes=67043328
        ),
    )(*args)


def solution(mesh):
    split = Mesh(
        mesh.devices.reshape(mesh.shape["dp"], 4, 4, 2, mesh.shape["tensor"]),
        ("dp", "seq_0", "seq_1", "seq_2", "tensor"),
    )
    placed = (
        P("dp", SEQ, "tensor"),
        P("dp", SEQ, "tensor"),
        P("dp", SEQ, "tensor"),
        P("dp", SEQ),
        P("dp", SEQ, "tensor"),
        P("dp", SEQ, "tensor"),
        P("dp", SEQ, "tensor"),
        P("dp", SEQ, None),
        P(None, "tensor"),
        P("dp", None),
        P("dp", None),
    )
    return jax.shard_map(
        on_device,
        mesh=split,
        in_specs=placed,
        out_specs=(P("dp", SEQ, "tensor"), P(DP_SEQ, "tensor")),
        check_vma=False,
    )
```
